512 devices in a mesh: ta: 64 (over z, y_lo, x), sa: 8 (over y_hi, core).
Axes of the slice: x: 4, y: 8 (y_hi: 4, y_lo: 2; y = y_hi * 2 + y_lo), z: 8, core: 2. Of those that a mesh axis runs over, the one named last changes fastest.
Arguments:
- rhs: float32 [1, 2, 40, 64, 8, 128], P(None, None, None, 'ta', 'sa'), may hold values from -6 to 6
- links: bfloat16 [4, 2, 40, 40, 64, 8, 128], P(None, None, None, None, 'ta', 'sa'), may hold values from -0.625 to 0.625
- clover: bfloat16 [2, 40, 40, 64, 8, 128], P(None, None, None, 'ta', 'sa'), may hold values from -1 to 7
- mr_steps: int32 [64, 8, 2], P('ta', 'sa'), may hold values from 2 to 3
Outputs:
- solution: float32 [1, 2, 40, 64, 8, 128], P(None, None, None, 'ta', 'sa')
- residual: float32 [1, 2, 40, 64, 8, 128], P(None, None, None, 'ta', 'sa')
The draws below stay inside these ranges and needn't reach their ends.
All inputs are finite; a program needn't handle non-finite values.
Results may differ from the reference program's by a relative error of at most 0.0003.
Values sent between devices are 32-bit elements; how exact they have to be, the bound alone decides.
A program may use at most 128 MiB of HBM per device.

```python
import jax
import jax.numpy as jnp
from jax import lax

NVEC = 20
DOF = 40
NRHS = 1
TD = 2
LZ = 4
LY = 4
LX = 4
MR_MAX = 3
SWEEPS = 2
NTD = 64
NZD = 8
DS = 128


def draw_clover(key, part):
    folded = jax.random.fold_in(key, 7)
    first, second = jax.random.split(folded)
    shape = (2, DOF, DOF, NTD, NZD, DS)
    spread = jax.random.normal(first, shape, jnp.float32) / jnp.sqrt(jnp.float32(DOF))
    diagonal = jax.random.uniform(second, (NTD, NZD, DS), jnp.float32, 3.5, 5.0)
    spread = jnp.clip(spread, -1.0, 1.0)
    identity = jnp.eye(DOF, dtype=jnp.float32)[:, :, None, None, None]
    real_part = spread[0] + identity * diagonal[None, None]
    return jnp.stack([real_part, spread[1]], 0).astype(jnp.bfloat16)


def with_ends(array, rng, low, largest):
    spot = [jax.random.randint(jax.random.fold_in(rng, axis), (), 0, length) for axis, length in enumerate(array.shape)]
    longest = array.shape.index(max(array.shape))
    neighbour = spot[:longest] + [(spot[longest] + 1) % array.shape[longest]] + spot[longest + 1:]
    return array.at[tuple(spot)].set(low).at[tuple(neighbour)].set(largest)


def levels(own_key, shape, cuts, smallest, top_value):
    factor_of = 1.0
    for axis_at, shards_of in cuts:
        draws = jax.random.uniform(jax.random.fold_in(jax.random.fold_in(own_key, 6), axis_at), (shards_of,), jnp.float32, smallest / len(cuts), top_value / len(cuts))
        factor_of = factor_of * jnp.repeat(jnp.exp(draws), shape[axis_at] // shards_of).reshape((-1,) + (1,) * (len(shape) - 1 - axis_at))
    return factor_of


def bell_draw(own_key, shape, deviation, most, cuts=(), kind=jnp.bfloat16):
    values = deviation * jax.random.normal(own_key, shape, jnp.float32)
    if cuts:
        values = values * levels(own_key, shape, cuts, -0.22, 0.18)
    return jnp.clip(values, -most, most).astype(kind)


def setup_inputs(seed: int = 0) -> dict:
    key_list = jax.random.split(jax.random.key(seed), 5)
    rhs = bell_draw(key_list[0], (NRHS, 2, DOF, NTD, NZD, DS), 1.0, 6.0, ((3, 64), (4, 8)), jnp.float32)
    links = bell_draw(key_list[1], (4, 2, DOF, DOF, NTD, NZD, DS), (2 * DOF) ** -0.5, 0.625, ((4, 64), (5, 8)))
    clover = draw_clover(jax.random.fold_in(key_list[4], 71), 0)
    mr_steps = with_ends(jax.random.randint(key_list[3], (NTD, NZD, 2), 2, MR_MAX + 1), jax.random.fold_in(key_list[3], 1), 2, MR_MAX).astype(jnp.int32)
    return {"rhs": rhs, "links": links, "clover": clover, "mr_steps": mr_steps}


HIGHEST = lax.Precision.HIGHEST


def complex_apply(matrices, vectors, dagger):
    real_mat = matrices[0].astype(jnp.float32)
    imag_mat = matrices[1].astype(jnp.float32)
    real_vec = vectors[:, 0]
    imag_vec = vectors[:, 1]
    pattern = "ji...,rj...->ri..." if dagger else "ij...,rj...->ri..."

    def product(left, right):
        return jnp.einsum(pattern, left, right, precision=HIGHEST)

    if dagger:
        real_out = product(real_mat, real_vec) + product(imag_mat, imag_vec)
        imag_out = product(real_mat, imag_vec) - product(imag_mat, real_vec)
    else:
        real_out = product(real_mat, real_vec) - product(imag_mat, imag_vec)
        imag_out = product(real_mat, imag_vec) + product(imag_mat, real_vec)
    return jnp.stack([real_out, imag_out], axis=1)


def lattice_view(field):
    leading = field.shape[:3]
    shaped = field.reshape(leading + (NTD, NZD, TD, LZ, LY, LX))
    shaped = jnp.transpose(shaped, (0, 1, 2, 3, 5, 4, 6, 7, 8))
    return shaped.reshape(leading + (NTD * TD, NZD * LZ, LY, LX))


def domain_view(lattice):
    leading = lattice.shape[:3]
    shaped = lattice.reshape(leading + (NTD, TD, NZD, LZ, LY, LX))
    shaped = jnp.transpose(shaped, (0, 1, 2, 3, 5, 4, 6, 7, 8))
    return shaped.reshape(leading + (NTD, NZD, DS))


def shifted(field, direction, amount):
    return domain_view(jnp.roll(lattice_view(field), amount, axis=3 + direction))


def apply_operator(field, links, clover):
    signs = jnp.where(jnp.arange(DOF) < NVEC, 1.0, -1.0).astype(jnp.float32)[:, None, None]

    def backward_terms(index):
        vectors = lax.dynamic_index_in_dim(field, index, 3, keepdims=False)
        matrices = lax.dynamic_index_in_dim(links, index, 4, keepdims=False)
        return jnp.stack([signs * complex_apply(matrices[direction], signs * vectors, True) for direction in range(4)], 0)

    back_terms = jnp.moveaxis(lax.map(backward_terms, jnp.arange(NTD)), 0, 4)
    neighbours = jnp.stack([shifted(field, direction, -1) for direction in range(4)], 0)
    behind_total = shifted(back_terms[0], 0, 1)
    for direction in range(1, 4):
        behind_total = behind_total + shifted(back_terms[direction], direction, 1)

    def forward_terms(index):
        vectors = lax.dynamic_index_in_dim(field, index, 3, keepdims=False)
        nearby = lax.dynamic_index_in_dim(neighbours, index, 4, keepdims=False)
        matrices = lax.dynamic_index_in_dim(links, index, 4, keepdims=False)
        self_block = lax.dynamic_index_in_dim(clover, index, 3, keepdims=False)
        total = complex_apply(self_block, vectors, False)
        for direction in range(4):
            total = total - complex_apply(matrices[direction], nearby[direction], False)
        return total

    result = jnp.moveaxis(lax.map(forward_terms, jnp.arange(NTD)), 0, 3)
    return result - behind_total


def block_sums(component):
    shaped = component.reshape(component.shape[:4] + (2, DS // 2))
    return jnp.sum(shaped, axis=(1, 5))


def block_scale(factor, component):
    shaped = component.reshape(component.shape[:4] + (2, DS // 2))
    return (factor[:, None, :, :, :, None] * shaped).reshape(component.shape)


def reference(rhs, links, clover, mr_steps):
    colour = (jnp.arange(DS)[None, :] // (DS // 2) + jnp.arange(NZD)[:, None]) % 2
    solution = jnp.zeros_like(rhs)
    for sweep_index in range(SWEEPS):
        for colour_index in range(2):
            mask = (colour == colour_index).astype(jnp.float32)
            remainder = rhs - apply_operator(solution, links, clover)
            search = remainder * mask
            correction = jnp.zeros_like(search)
            for step_index in range(MR_MAX):
                image = apply_operator(search, links, clover) * mask
                real_s = search[:, 0]
                imag_s = search[:, 1]
                real_q = image[:, 0]
                imag_q = image[:, 1]
                numer_real = block_sums(real_q * real_s + imag_q * imag_s)
                numer_imag = block_sums(real_q * imag_s - imag_q * real_s)
                denom = block_sums(real_q * real_q + imag_q * imag_q) + 1e-6
                live = (step_index < mr_steps)[None]
                alpha_real = jnp.where(live, numer_real / denom, 0.0)
                alpha_imag = jnp.where(live, numer_imag / denom, 0.0)
                correction = correction + jnp.stack([block_scale(alpha_real, real_s) - block_scale(alpha_imag, imag_s), block_scale(alpha_real, imag_s) + block_scale(alpha_imag, real_s)], 1)
                search = search - jnp.stack([block_scale(alpha_real, real_q) - block_scale(alpha_imag, imag_q), block_scale(alpha_real, imag_q) + block_scale(alpha_imag, real_q)], 1)
            solution = solution + correction
    residual = rhs - apply_operator(solution, links, clover)
    return solution, residual
```

```python
import functools

import jax
import jax.numpy as jnp
from jax import lax
from jax.experimental import pallas as pl
from jax.experimental.pallas import tpu as pltpu
from jax.sharding import PartitionSpec as P

MESH = pl.DeviceIdType.MESH
MR_MAX = 3
HALF_SWEEPS = 4
DOF = 40
PAIRS = 20
LANES = 128
HALF = 64
CLOVER, ZDIR, YDIR, XDIR, TDIR = 0, 1, 2, 3, 4
LINK_OF = {TDIR: 0, ZDIR: 1, YDIR: 2, XDIR: 3}


def roll(x, amount):
    return pltpu.roll(x, amount % LANES, axis=1)


def fold_rows(x):
    return x[0:8] + x[8:16] + x[16:24] + x[24:32] + x[32:40]


def kernel(
    time_count,
    space_count,
    rhs_ref,
    links_ref,
    clover_ref,
    steps_ref,
    sol_ref,
    res_ref,
    raw,
    mat_a,
    mat_b,
    mat_s,
    resid,
    solu,
    search,
    corr,
    face,
    bcast,
    fwd_re,
    fwd_im,
    tsend,
    zup_send,
    zdn_send,
    trecv,
    zup_recv,
    zdn_recv,
    load_sem,
    send_sem,
    recv_sem,
):
    f32 = jnp.float32
    tpos = lax.axis_index("ta")
    zpos = lax.axis_index("sa")
    t_up = lax.rem(tpos + 1, time_count)
    t_dn = lax.rem(tpos + time_count - 1, time_count)
    z_up = lax.rem(zpos + 1, space_count)
    z_dn = lax.rem(zpos + space_count - 1, space_count)

    def load(mat):
        source = clover_ref if mat == CLOVER else links_ref.at[LINK_OF[mat]]
        return pltpu.make_async_copy(source, raw.at[mat], load_sem.at[mat])

    for mat in (CLOVER, ZDIR, YDIR, XDIR, TDIR):
        load(mat).start()
    barrier = pltpu.get_barrier_semaphore()
    for target in ((t_up, zpos), (t_dn, zpos), (tpos, z_up), (tpos, z_dn)):
        pl.semaphore_signal(barrier, inc=1, device_id=target, device_id_type=MESH)

    lane = lax.broadcasted_iota(jnp.int32, (DOF, LANES), 1)
    row = lax.broadcasted_iota(jnp.int32, (DOF, LANES), 0)
    low = lane < HALF
    site = lane % HALF
    x_at = site % 4
    y_at = (site // 4) % 4
    z_at = site // 16
    sign = jnp.where(row < DOF // 2, 1.0, -1.0).astype(f32)
    low8 = low[0:8]
    tail_keep = (low8 & (row[0:8] < 4)) | (jnp.logical_not(low8) & (row[0:8] >= 4))

    def pack(mat, half):
        keep = low if False else ((lane // HALF) == half)
        first = half == 0

        def one(i, carry):
            group = i // 8
            lo_row = i + 8 * group
            hi_row = lo_row + 8 - 4 * (group // 2)
            parts = []
            for comp in range(2):
                upper = raw[mat, comp, lo_row].astype(f32)
                lower = raw[mat, comp, hi_row].astype(f32)
                mixed = roll(jnp.where(low, lower, upper), HALF)
                own = jnp.where(first, upper, lower)
                parts.append(jnp.where(keep, own, mixed))
            mat_a[half, mat, i] = parts[0]
            mat_b[half, mat, i] = parts[1]
            mat_s[half, mat, i] = parts[0] + parts[1]
            return carry

        lax.fori_loop(0, PAIRS, one, 0, unroll=2)

    def dup(x, half):
        return jnp.where((lane // HALF) == half, x, roll(x, HALF))

    def split_dup(x):
        turned = roll(x, HALF)
        return jnp.where(low, x, turned), jnp.where(low, turned, x)

    def store_bcast(re, im):
        def packed(v):
            tail = v[32:40]
            return jnp.concatenate(
                [
                    jnp.where(low8, v[0:8], v[8:16]),
                    jnp.where(low8, v[16:24], v[24:32]),
                    jnp.where(low8, tail, pltpu.roll(tail, 4, axis=0)),
                ],
                axis=0,
            )

        wr = packed(re * sign)
        wi = packed(im * sign)
        bcast[0] = wr
        bcast[1] = -(wr + wi)
        bcast[2] = wr - wi

    def combos(re, im):
        return re, im - re, re + im

    def forward(i, mats, vec, fresh):
        k1 = fold_rows(mats[2] * vec[0])
        k2 = fold_rows(mats[0] * vec[1])
        k3 = fold_rows(mats[1] * vec[2])
        if fresh:
            fwd_re[i] = k1 - k3
            fwd_im[i] = k1 + k2
        else:
            fwd_re[i] = fwd_re[i] + (k1 - k3)
            fwd_im[i] = fwd_im[i] + (k1 + k2)

    def get(half, mat, i):
        return mat_a[half, mat, i], mat_b[half, mat, i], mat_s[half, mat, i]

    def forward_only(half, mat, re, im, fresh):
        vec = combos(re, im)

        def one(i, carry):
            forward(i, get(half, mat, i), vec, fresh)
            return carry

        lax.fori_loop(0, PAIRS, one, 0, unroll=4)

    def accumulate(i, mats, acc):
        w1 = bcast[0, pl.ds(i, 1), :]
        w2 = bcast[1, pl.ds(i, 1), :]
        w3 = bcast[2, pl.ds(i, 1), :]
        return acc[0] + mats[2] * w1, acc[1] + mats[0] * w2, acc[2] + mats[1] * w3

    def finish(acc):
        return sign * (acc[0] - acc[2]), -sign * (acc[0] + acc[1])

    zeros3 = (jnp.zeros((DOF, LANES), f32),) * 3

    def both(half, mat, re, im):
        vec = combos(re, im)

        def one(i, acc):
            mats = get(half, mat, i)
            forward(i, mats, vec, False)
            return accumulate(i, mats, acc)

        return finish(lax.fori_loop(0, PAIRS, one, zeros3, unroll=4))

    def backward_only(half, mat):
        def one(i, acc):
            return accumulate(i, get(half, mat, i), acc)

        return finish(lax.fori_loop(0, PAIRS, one, zeros3, unroll=4))

    def gather_forward(ref):
        groups = []
        for start, count in ((0, 8), (8, 8), (16, 4)):
            rows = jnp.sum(ref[start : start + count], axis=1)
            if count == 4:
                rows = jnp.concatenate([rows, rows], axis=0)
            turned = roll(rows, HALF)
            if count == 8:
                groups.append(jnp.where(low8, rows, turned))
                groups.append(jnp.where(low8, turned, rows))
            else:
                groups.append(jnp.where(tail_keep, rows, turned))
        return jnp.concatenate(groups, axis=0)

    def total(x):
        lanes = jnp.broadcast_to(jnp.sum(fold_rows(x), axis=1, keepdims=True), (8, LANES))
        lanes = lanes + pltpu.roll(lanes, 4, axis=0)
        lanes = lanes + pltpu.roll(lanes, 2, axis=0)
        lanes = lanes + pltpu.roll(lanes, 1, axis=0)
        return 0.5 * lanes

    def spread(x):
        return jnp.concatenate([x] * 5, axis=0)

    def mr_step(half, step):
        sr, si = search[0], search[1]
        store_bcast(sr, si)
        forward_only(half, CLOVER, sr, si, True)

        def ahead(v, mat):
            if mat == ZDIR:
                return jnp.where(z_at == 3, 0.0, -roll(v, -16))
            if mat == YDIR:
                return -jnp.where(y_at == 3, roll(v, 12), roll(v, -4))
            return -jnp.where(x_at == 3, roll(v, 3), roll(v, -1))

        zr, zi = both(half, ZDIR, ahead(sr, ZDIR), ahead(si, ZDIR))
        zr, zi = roll(zr, 16), roll(zi, 16)
        yr, yi = both(half, YDIR, ahead(sr, YDIR), ahead(si, YDIR))
        xr, xi = both(half, XDIR, ahead(sr, XDIR), ahead(si, XDIR))

        def behind(z, y, x):
            y = jnp.where(y_at == 0, roll(y, -12), roll(y, 4))
            x = jnp.where(x_at == 0, roll(x, -3), roll(x, 1))
            out = jnp.where(z_at == 0, 0.0, z) + y + x
            return out + roll(out, HALF)

        qr = gather_forward(fwd_re) - behind(zr, yr, xr)
        qi = gather_forward(fwd_im) - behind(zi, yi, xi)
        nr = total(qr * sr + qi * si)
        ni = total(qr * si - qi * sr)
        inv = 1.0 / (total(qr * qr + qi * qi) + 1e-6)
        live = step < steps_ref[half]
        ar = spread(jnp.where(live, nr * inv, 0.0))
        ai = spread(jnp.where(live, ni * inv, 0.0))
        corr[0] = corr[0] + (ar * sr - ai * si)
        corr[1] = corr[1] + (ar * si + ai * sr)
        face[0] = face[0] + (ar * zr - ai * zi)
        face[1] = face[1] + (ar * zi + ai * zr)
        search[0] = sr - (ar * qr - ai * qi)
        search[1] = si - (ar * qi + ai * qr)

    first_half = lax.rem(zpos, 2)
    for comp in range(2):
        full = rhs_ref[comp]
        for half in range(2):
            resid[half, comp] = dup(full, half)
            solu[half, comp] = jnp.zeros((DOF, LANES), f32)

    for mat in (CLOVER, ZDIR, YDIR, XDIR, TDIR):
        load(mat).wait()
        pack(mat, first_half)

    pl.semaphore_wait(barrier, 4)

    def copies(turn, t_to):
        t_copy = pltpu.make_async_remote_copy(
            src_ref=tsend.at[turn],
            dst_ref=trecv.at[turn],
            send_sem=send_sem.at[turn, 0],
            recv_sem=recv_sem.at[turn, 0],
            device_id=(t_to, zpos),
            device_id_type=MESH,
        )
        up_copy = pltpu.make_async_remote_copy(
            src_ref=zup_send.at[turn],
            dst_ref=zup_recv.at[turn],
            send_sem=send_sem.at[turn, 1],
            recv_sem=recv_sem.at[turn, 1],
            device_id=(tpos, z_up),
            device_id_type=MESH,
        )
        dn_copy = pltpu.make_async_remote_copy(
            src_ref=zdn_send.at[turn],
            dst_ref=zdn_recv.at[turn],
            send_sem=send_sem.at[turn, 2],
            recv_sem=recv_sem.at[turn, 2],
            device_id=(tpos, z_dn),
            device_id_type=MESH,
        )
        return t_copy, up_copy, dn_copy

    def half_sweep(turn, carry):
        half = lax.rem(turn + zpos, 2)
        other = 1 - half
        t_to = jnp.where(half == 0, t_dn, t_up)
        t_copy, up_copy, dn_copy = copies(turn, t_to)
        for comp in range(2):
            search[comp] = resid[half, comp]
            corr[comp] = jnp.zeros((DOF, LANES), f32)
            face[comp] = jnp.zeros((DOF, LANES), f32)

        def step(k, c):
            mr_step(half, k)
            return c

        lax.fori_loop(0, MR_MAX, step, 0)
        er, ei = corr[0], corr[1]
        zdn_send[turn] = roll(jnp.where(low, ei, er), -16)
        dn_copy.start()
        fr, fi = face[0], face[1]
        fr = fr + roll(fr, HALF)
        fi = fi + roll(fi, HALF)
        zup_send[turn] = jnp.where(low, fr, fi)
        up_copy.start()
        store_bcast(er, ei)

        @pl.when(half == 0)
        def _():
            tsend[turn] = jnp.where(low, er, ei)
            t_copy.start()

        pr, pi = backward_only(half, TDIR)
        pr = pr + roll(pr, HALF)
        pi = pi + roll(pi, HALF)

        @pl.when(half == 1)
        def _():
            tsend[turn] = jnp.where(low, pr, pi)
            t_copy.start()

        for comp in range(2):
            resid[half, comp] = search[comp]
            solu[half, comp] = solu[half, comp] + corr[comp]
        face[0] = pr
        face[1] = pi

        @pl.when(turn == 0)
        def _():
            for mat in (TDIR, ZDIR, CLOVER, YDIR, XDIR):
                pack(mat, other)

        @pl.when(half == 1)
        def _():
            forward_only(other, TDIR, corr[0], corr[1], True)

        t_copy.wait_recv()

        @pl.when(half == 0)
        def _():
            tr, ti = split_dup(trecv[turn])
            forward_only(other, TDIR, tr, ti, True)

        @pl.when(half == 1)
        def _():
            tr, ti = split_dup(trecv[turn])
            face[0] = tr
            face[1] = ti

        dn_copy.wait_recv()
        zr, zi = split_dup(zdn_recv[turn])
        forward_only(
            other,
            ZDIR,
            jnp.where(z_at == 3, zr, 0.0),
            jnp.where(z_at == 3, zi, 0.0),
            False,
        )
        up_copy.wait_recv()
        ur, ui = split_dup(zup_recv[turn])
        ur = jnp.where(z_at == 0, ur, 0.0)
        ui = jnp.where(z_at == 0, ui, 0.0)
        resid[other, 0] = resid[other, 0] + gather_forward(fwd_re) + face[0] + ur
        resid[other, 1] = resid[other, 1] + gather_forward(fwd_im) + face[1] + ui
        return carry

    lax.fori_loop(0, HALF_SWEEPS, half_sweep, 0)

    for comp in range(2):
        sol_ref[comp] = jnp.where(low, solu[0, comp], solu[1, comp])
        res_ref[comp] = jnp.where(low, resid[0, comp], resid[1, comp])

    def drain(turn, carry):
        for copy in copies(turn, t_up):
            copy.wait_send()
        return carry

    lax.fori_loop(0, HALF_SWEEPS, drain, 0)


def solution(mesh):
    time_count, space_count = mesh.shape["ta"], mesh.shape["sa"]
    f32 = jnp.float32
    vmem = pltpu.VMEM
    field = (2, DOF, LANES)

    def shards(rhs, links, clover, mr_steps):
        out = jax.ShapeDtypeStruct(field, f32)
        packed = vmem((2, 5, PAIRS, DOF, LANES), f32)
        message = vmem((HALF_SWEEPS, DOF, LANES), f32)
        sol, res = pl.pallas_call(
            functools.partial(kernel, time_count, space_count),
            out_shape=(out, out),
            in_specs=[
                pl.BlockSpec(memory_space=pltpu.VMEM),
                pl.BlockSpec(memory_space=pl.ANY),
                pl.BlockSpec(memory_space=pl.ANY),
                pl.BlockSpec(memory_space=pltpu.SMEM),
            ],
            out_specs=(pl.BlockSpec(memory_space=pltpu.VMEM),) * 2,
            scratch_shapes=[
                vmem((5, 2, DOF, DOF, LANES), jnp.bfloat16),
                packed,
                packed,
                packed,
                vmem((2,) + field, f32),
                vmem((2,) + field, f32),
                vmem(field, f32),
                vmem(field, f32),
                vmem(field, f32),
                vmem((3, 24, LANES), f32),
                vmem((PAIRS, 8, LANES), f32),
                vmem((PAIRS, 8, LANES), f32),
                message,
                message,
                message,
                message,
                message,
                message,
                pltpu.SemaphoreType.DMA((5,)),
                pltpu.SemaphoreType.DMA((HALF_SWEEPS, 3)),
                pltpu.SemaphoreType.DMA((HALF_SWEEPS, 3)),
            ],
            compiler_params=pltpu.CompilerParams(
                collective_id=0, has_side_effects=True, vmem_limit_bytes=50 * 2**20
            ),
        )(
            rhs.reshape(field),
            links.reshape(4, 2, DOF, DOF, LANES),
            clover.reshape(2, DOF, DOF, LANES),
            mr_steps.reshape(2),
        )
        shape = rhs.shape
        return sol.reshape(shape), res.reshape(shape)

    placed = (
        P(None, None, None, "ta", "sa", None),
        P(None, None, None, None, "ta", "sa", None),
        P(None, None, None, "ta", "sa", None),
        P("ta", "sa", None),
    )
    return jax.shard_map(
        shards,
        mesh=mesh,
        in_specs=placed,
        out_specs=(P(None, None, None, "ta", "sa", None),) * 2,
        check_vma=False,
    )
```

```python
import functools

import jax
import jax.numpy as jnp
from jax import lax
from jax.experimental import pallas as pl
from jax.experimental.pallas import tpu as pltpu
from jax.sharding import PartitionSpec as P

MESH = pl.DeviceIdType.MESH
MR_MAX = 3
HALF_SWEEPS = 4
DOF = 40
PAIRS = 20
LANES = 128
HALF = 64
CLOVER, ZDIR, YDIR, XDIR, TDIR = 0, 1, 2, 3, 4
LINK_OF = {TDIR: 0, ZDIR: 1, YDIR: 2, XDIR: 3}


def roll(x, amount):
    return pltpu.roll(x, amount % LANES, axis=1)


def fold_rows(x):
    return x[0:8] + x[8:16] + x[16:24] + x[24:32] + x[32:40]


def kernel(
    time_count,
    space_count,
    rhs_hbm,
    links_ref,
    clover_ref,
    steps_ref,
    sol_ref,
    res_ref,
    mats,
    raw,
    resid,
    solu,
    state,
    bcast,
    fwd_re,
    fwd_im,
    tsend,
    zup_send,
    zdn_send,
    trecv,
    zup_recv,
    zdn_recv,
    load_sem,
    send_sem,
    recv_sem,
):
    f32 = jnp.float32
    search, corr, face, rhs_ref = (state.at[pl.ds(2 * k, 2)] for k in range(4))
    tpos = lax.axis_index("ta")
    zpos = lax.axis_index("sa")
    t_up = lax.rem(tpos + 1, time_count)
    t_dn = lax.rem(tpos + time_count - 1, time_count)
    z_up = lax.rem(zpos + 1, space_count)
    z_dn = lax.rem(zpos + space_count - 1, space_count)

    def load(mat):
        source = clover_ref if mat == CLOVER else links_ref.at[LINK_OF[mat]]
        return pltpu.make_async_copy(source, raw.at[mat], load_sem.at[mat])

    rhs_load = pltpu.make_async_copy(rhs_hbm, rhs_ref, load_sem.at[5])
    rhs_load.start()
    for mat in (CLOVER, ZDIR, YDIR, XDIR, TDIR):
        load(mat).start()
    barrier = pltpu.get_barrier_semaphore()
    for target in ((t_up, zpos), (t_dn, zpos), (tpos, z_up), (tpos, z_dn)):
        pl.semaphore_signal(barrier, inc=1, device_id=target, device_id_type=MESH)

    lane = lax.broadcasted_iota(jnp.int32, (DOF, LANES), 1)
    row = lax.broadcasted_iota(jnp.int32, (DOF, LANES), 0)
    low = lane < HALF
    site = lane % HALF
    x_at = site % 4
    y_at = (site // 4) % 4
    z_at = site // 16
    sign = jnp.where(row < DOF // 2, 1.0, -1.0).astype(f32)
    low8 = low[0:8]
    tail_keep = (low8 & (row[0:8] < 4)) | (jnp.logical_not(low8) & (row[0:8] >= 4))

    def pack(mat, half):
        source = lax.broadcasted_iota(jnp.int32, (2 * LANES, LANES), 0)
        target = lax.broadcasted_iota(jnp.int32, (2 * LANES, LANES), 1)
        wanted = (target // HALF) * LANES + half * HALF + target % HALF
        select = jnp.where(source == wanted, 1.0, 0.0).astype(jnp.bfloat16)
        for out_at, lo_at, hi_at, count in ((0, 0, 8, 8), (8, 16, 24, 8), (16, 32, 36, 4)):
            parts = []
            for comp in range(2):
                upper = raw[mat, comp, lo_at : lo_at + count].reshape(count * DOF, LANES)
                lower = raw[mat, comp, hi_at : hi_at + count].reshape(count * DOF, LANES)
                both_rows = jnp.concatenate([upper, lower], axis=1)
                out = jnp.dot(both_rows, select, preferred_element_type=f32)
                parts.append(out.reshape(count, DOF, LANES))
            mats[half, mat, out_at : out_at + count, 0] = parts[0]
            mats[half, mat, out_at : out_at + count, 1] = parts[1]
            mats[half, mat, out_at : out_at + count, 2] = parts[0] + parts[1]

    def dup(x, half):
        return jnp.where((lane // HALF) == half, x, roll(x, HALF))

    def split_dup(x):
        turned = roll(x, HALF)
        return jnp.where(low, x, turned), jnp.where(low, turned, x)

    def store_bcast(re, im):
        def packed(v):
            tail = v[32:40]
            return jnp.concatenate(
                [
                    jnp.where(low8, v[0:8], v[8:16]),
                    jnp.where(low8, v[16:24], v[24:32]),
                    jnp.where(low8, tail, pltpu.roll(tail, 4, axis=0)),
                ],
                axis=0,
            )

        wr = packed(re * sign)
        wi = packed(im * sign)
        bcast[0, 0:24] = wr
        bcast[1, 0:24] = -(wr + wi)
        bcast[2, 0:24] = wr - wi

    def combos(re, im):
        return re, im - re, re + im

    def forward(i, block, vec, fresh):
        k1 = fold_rows(block[2] * vec[0])
        k2 = fold_rows(block[0] * vec[1])
        k3 = fold_rows(block[1] * vec[2])
        if fresh:
            fwd_re[i] = k1 - k3
            fwd_im[i] = k1 + k2
        else:
            fwd_re[i] = fwd_re[i] + (k1 - k3)
            fwd_im[i] = fwd_im[i] + (k1 + k2)

    def get(half, mat, i):
        return tuple(mats[half, mat, i, k] for k in range(3))

    def forward_only(half, mat, re, im, fresh):
        vec = combos(re, im)

        def one(i, carry):
            forward(i, get(half, mat, i), vec, fresh)
            return carry

        lax.fori_loop(0, PAIRS, one, 0, unroll=20)

    def accumulate(i, block, acc):
        w1 = bcast[0, pl.ds(i, 1), :]
        w2 = bcast[1, pl.ds(i, 1), :]
        w3 = bcast[2, pl.ds(i, 1), :]
        return acc[0] + block[2] * w1, acc[1] + block[0] * w2, acc[2] + block[1] * w3

    def finish(acc):
        return sign * (acc[0] - acc[2]), -sign * (acc[0] + acc[1])

    zeros3 = (jnp.zeros((DOF, LANES), f32),) * 3

    def both(half, mat, re, im):
        vec = combos(re, im)

        def one(i, acc):
            block = get(half, mat, i)
            forward(i, block, vec, False)
            return accumulate(i, block, acc)

        return finish(lax.fori_loop(0, PAIRS, one, zeros3, unroll=20))

    def backward_only(half, mat):
        def one(i, acc):
            return accumulate(i, get(half, mat, i), acc)

        return finish(lax.fori_loop(0, PAIRS, one, zeros3, unroll=20))

    sub = lax.broadcasted_iota(jnp.int32, (8, LANES), 0)

    def pair(lo, hi, width):
        keep = (sub & width) == 0
        return jnp.where(keep, lo, hi) + pltpu.roll(jnp.where(keep, hi, lo), width, axis=0)

    def fold_eight(tiles):
        ones = [pair(tiles[2 * k], tiles[2 * k + 1], 1) for k in range(4)]
        twos = [pair(ones[2 * k], ones[2 * k + 1], 2) for k in range(2)]
        return pair(twos[0], twos[1], 4)

    def gather_forward(ref):
        groups = []
        for start in (0, 8, 16):
            if start < 16:
                rows = fold_eight([ref[start + k] for k in range(8)])
            else:
                rows = fold_eight([ref[start + k % 4] for k in range(8)])
            turned = roll(rows, HALF)
            if start < 16:
                groups.append(jnp.where(low8, rows, turned))
                groups.append(jnp.where(low8, turned, rows))
            else:
                groups.append(jnp.where(tail_keep, rows, turned))
        return jnp.concatenate(groups, axis=0)

    def total(x):
        lanes = jnp.broadcast_to(jnp.sum(fold_rows(x), axis=1, keepdims=True), (8, LANES))
        lanes = lanes + pltpu.roll(lanes, 4, axis=0)
        lanes = lanes + pltpu.roll(lanes, 2, axis=0)
        lanes = lanes + pltpu.roll(lanes, 1, axis=0)
        return 0.5 * lanes

    def spread(x):
        return jnp.concatenate([x] * 5, axis=0)

    def mr_step(half, step):
        sr, si = search[0], search[1]
        store_bcast(sr, si)
        forward_only(half, CLOVER, sr, si, True)

        def ahead(v, mat):
            if mat == ZDIR:
                return jnp.where(z_at == 3, 0.0, -roll(v, -16))
            if mat == YDIR:
                return -jnp.where(y_at == 3, roll(v, 12), roll(v, -4))
            return -jnp.where(x_at == 3, roll(v, 3), roll(v, -1))

        zr, zi = both(half, ZDIR, ahead(sr, ZDIR), ahead(si, ZDIR))
        zr, zi = roll(zr, 16), roll(zi, 16)
        yr, yi = both(half, YDIR, ahead(sr, YDIR), ahead(si, YDIR))
        xr, xi = both(half, XDIR, ahead(sr, XDIR), ahead(si, XDIR))

        def behind(z, y, x):
            y = jnp.where(y_at == 0, roll(y, -12), roll(y, 4))
            x = jnp.where(x_at == 0, roll(x, -3), roll(x, 1))
            out = jnp.where(z_at == 0, 0.0, z) + y + x
            return out + roll(out, HALF)

        qr = gather_forward(fwd_re) - behind(zr, yr, xr)
        qi = gather_forward(fwd_im) - behind(zi, yi, xi)
        nr = total(qr * sr + qi * si)
        ni = total(qr * si - qi * sr)
        inv = 1.0 / (total(qr * qr + qi * qi) + 1e-6)
        live = step < steps_ref[half]
        ar = spread(jnp.where(live, nr * inv, 0.0))
        ai = spread(jnp.where(live, ni * inv, 0.0))
        corr[0] = corr[0] + (ar * sr - ai * si)
        corr[1] = corr[1] + (ar * si + ai * sr)
        face[0] = face[0] + (ar * zr - ai * zi)
        face[1] = face[1] + (ar * zi + ai * zr)
        search[0] = sr - (ar * qr - ai * qi)
        search[1] = si - (ar * qi + ai * qr)

    first_half = lax.rem(zpos, 2)
    rhs_load.wait()
    for comp in range(2):
        full = rhs_ref[comp]
        for half in range(2):
            resid[half, comp] = dup(full, half)
            solu[half, comp] = jnp.zeros((DOF, LANES), f32)

    for mat in (CLOVER, ZDIR, YDIR, XDIR, TDIR):
        load(mat).wait()
        pack(mat, first_half)

    def copies(turn, t_to):
        t_copy = pltpu.make_async_remote_copy(
            src_ref=tsend.at[turn],
            dst_ref=trecv.at[turn],
            send_sem=send_sem.at[turn, 0],
            recv_sem=recv_sem.at[turn, 0],
            device_id=(t_to, zpos),
            device_id_type=MESH,
        )
        up_copy = pltpu.make_async_remote_copy(
            src_ref=zup_send.at[turn],
            dst_ref=zup_recv.at[turn],
            send_sem=send_sem.at[turn, 1],
            recv_sem=recv_sem.at[turn, 1],
            device_id=(tpos, z_up),
            device_id_type=MESH,
        )
        dn_copy = pltpu.make_async_remote_copy(
            src_ref=zdn_send.at[turn],
            dst_ref=zdn_recv.at[turn],
            send_sem=send_sem.at[turn, 2],
            recv_sem=recv_sem.at[turn, 2],
            device_id=(tpos, z_dn),
            device_id_type=MESH,
        )
        return t_copy, up_copy, dn_copy

    def half_sweep(turn, carry):
        half = lax.rem(turn + zpos, 2)
        other = 1 - half
        t_to = jnp.where(half == 0, t_dn, t_up)
        t_copy, up_copy, dn_copy = copies(turn, t_to)
        for comp in range(2):
            search[comp] = resid[half, comp]
            corr[comp] = jnp.zeros((DOF, LANES), f32)
            face[comp] = jnp.zeros((DOF, LANES), f32)

        def step(k, c):
            mr_step(half, k)
            return c

        lax.fori_loop(0, MR_MAX, step, 0)

        @pl.when(turn == 0)
        def _():
            pl.semaphore_wait(barrier, 4)

        er, ei = corr[0], corr[1]

        @pl.when(half == 0)
        def _():
            tsend[turn] = jnp.where(low, er, ei)
            t_copy.start()

        zdn_send[turn] = roll(jnp.where(low, ei, er), -16)
        fr, fi = face[0], face[1]
        fr = fr + roll(fr, HALF)
        fi = fi + roll(fi, HALF)
        zup_send[turn] = jnp.where(low, fr, fi)
        dn_copy.start()
        up_copy.start()
        store_bcast(er, ei)
        pr, pi = backward_only(half, TDIR)
        pr = pr + roll(pr, HALF)
        pi = pi + roll(pi, HALF)

        @pl.when(half == 1)
        def _():
            tsend[turn] = jnp.where(low, pr, pi)
            t_copy.start()

        for comp in range(2):
            resid[half, comp] = search[comp]
            solu[half, comp] = solu[half, comp] + corr[comp]
        face[0] = pr
        face[1] = pi

        @pl.when(turn == 0)
        def _():
            for mat in (TDIR, ZDIR, CLOVER, YDIR, XDIR):
                pack(mat, other)

        dn_copy.wait_recv()
        zr, zi = split_dup(zdn_recv[turn])
        forward_only(
            other,
            ZDIR,
            jnp.where(z_at == 3, zr, 0.0),
            jnp.where(z_at == 3, zi, 0.0),
            True,
        )

        @pl.when(half == 1)
        def _():
            forward_only(other, TDIR, corr[0], corr[1], False)

        up_copy.wait_recv()
        ur, ui = split_dup(zup_recv[turn])
        ur = jnp.where(z_at == 0, ur, 0.0) + resid[other, 0]
        ui = jnp.where(z_at == 0, ui, 0.0) + resid[other, 1]

        @pl.when(half == 1)
        def _():
            resid[other, 0] = ur + gather_forward(fwd_re)
            resid[other, 1] = ui + gather_forward(fwd_im)

        @pl.when(half == 0)
        def _():
            resid[other, 0] = ur + face[0]
            resid[other, 1] = ui + face[1]

        t_copy.wait_recv()
        tr, ti = split_dup(trecv[turn])

        @pl.when(half == 0)
        def _():
            forward_only(other, TDIR, tr, ti, False)
            resid[other, 0] = resid[other, 0] + gather_forward(fwd_re)
            resid[other, 1] = resid[other, 1] + gather_forward(fwd_im)

        @pl.when(half == 1)
        def _():
            resid[other, 0] = resid[other, 0] + tr
            resid[other, 1] = resid[other, 1] + ti

        return carry

    lax.fori_loop(0, HALF_SWEEPS, half_sweep, 0)

    for comp in range(2):
        sol_ref[comp] = jnp.where(low, solu[0, comp], solu[1, comp])
        res_ref[comp] = jnp.where(low, resid[0, comp], resid[1, comp])

    def drain(turn, carry):
        for copy in copies(turn, t_up):
            copy.wait_send()
        return carry

    lax.fori_loop(0, HALF_SWEEPS, drain, 0)


def solution(mesh):
    time_count, space_count = mesh.shape["ta"], mesh.shape["sa"]
    f32 = jnp.float32
    vmem = pltpu.VMEM
    field = (2, DOF, LANES)

    def shards(rhs, links, clover, mr_steps):
        out = jax.ShapeDtypeStruct(field, f32)
        message = vmem((HALF_SWEEPS, DOF, LANES), f32)
        sol, res = pl.pallas_call(
            functools.partial(kernel, time_count, space_count),
            out_shape=(out, out),
            in_specs=[
                pl.BlockSpec(memory_space=pltpu.HBM),
                pl.BlockSpec(memory_space=pltpu.HBM),
                pl.BlockSpec(memory_space=pltpu.HBM),
                pl.BlockSpec(memory_space=pltpu.SMEM),
            ],
            out_specs=(pl.BlockSpec(memory_space=pltpu.VMEM),) * 2,
            scratch_shapes=[
                vmem((2, 5, PAIRS, 3, DOF, LANES), f32),
                vmem((5, 2, DOF, DOF, LANES), jnp.bfloat16),
                vmem((2,) + field, f32),
                vmem((2,) + field, f32),
                vmem((8, DOF, LANES), f32),
                vmem((3, 32, LANES), f32),
                vmem((PAIRS, 8, LANES), f32),
                vmem((PAIRS, 8, LANES), f32),
                message,
                message,
                message,
                message,
                message,
                message,
                pltpu.SemaphoreType.DMA((6,)),
                pltpu.SemaphoreType.DMA((HALF_SWEEPS, 3)),
                pltpu.SemaphoreType.DMA((HALF_SWEEPS, 3)),
            ],
            compiler_params=pltpu.CompilerParams(
                collective_id=0, has_side_effects=True, vmem_limit_bytes=67043328
            ),
        )(
            rhs.reshape(field),
            links.reshape(4, 2, DOF, DOF, LANES),
            clover.reshape(2, DOF, DOF, LANES),
            mr_steps.reshape(2),
        )
        shape = rhs.shape
        return sol.reshape(shape), res.reshape(shape)

    placed = (
        P(None, None, None, "ta", "sa", None),
        P(None, None, None, None, "ta", "sa", None),
        P(None, None, None, "ta", "sa", None),
        P("ta", "sa", None),
    )
    return jax.shard_map(
        shards,
        mesh=mesh,
        in_specs=placed,
        out_specs=(P(None, None, None, "ta", "sa", None),) * 2,
        check_vma=False,
    )
```

```python
import functools

import jax
import jax.numpy as jnp
from jax import lax
from jax.experimental import pallas as pl
from jax.experimental.pallas import tpu as pltpu
from jax.sharding import PartitionSpec as P

MESH = pl.DeviceIdType.MESH
MR_MAX = 3
HALF_SWEEPS = 4
DOF = 40
PAIRS = 20
LANES = 128
HALF = 64
CLOVER, ZDIR, YDIR, XDIR, TDIR = 0, 1, 2, 3, 4
LINK_OF = {TDIR: 0, ZDIR: 1, YDIR: 2, XDIR: 3}


def roll(x, amount):
    return pltpu.roll(x, amount % LANES, axis=1)


def fold_rows(x):
    return x[0:8] + x[8:16] + x[16:24] + x[24:32] + x[32:40]


def kernel(
    time_count,
    space_count,
    rhs_hbm,
    links_ref,
    clover_ref,
    steps_hbm,
    sol_ref,
    res_ref,
    mats,
    raw,
    resid,
    solu,
    state,
    bcast,
    fwd_re,
    fwd_im,
    tsend,
    zup_send,
    zdn_send,
    trecv,
    zup_recv,
    zdn_recv,
    steps_ref,
    load_sem,
    send_sem,
    recv_sem,
):
    f32 = jnp.float32
    search, corr, face, rhs_ref = (state.at[pl.ds(2 * k, 2)] for k in range(4))
    tpos = lax.axis_index("ta")
    zpos = lax.axis_index("sa")
    t_up = lax.rem(tpos + 1, time_count)
    t_dn = lax.rem(tpos + time_count - 1, time_count)
    z_up = lax.rem(zpos + 1, space_count)
    z_dn = lax.rem(zpos + space_count - 1, space_count)

    def load(mat):
        source = clover_ref if mat == CLOVER else links_ref.at[LINK_OF[mat]]
        return pltpu.make_async_copy(source, raw.at[mat], load_sem.at[mat])

    rhs_load = pltpu.make_async_copy(rhs_hbm, rhs_ref, load_sem.at[5])
    rhs_load.start()
    steps_load = pltpu.make_async_copy(steps_hbm, steps_ref, load_sem.at[6])
    steps_load.start()
    for mat in (CLOVER, ZDIR, YDIR, XDIR, TDIR):
        load(mat).start()
    barrier = pltpu.get_barrier_semaphore()
    for target in ((t_up, zpos), (t_dn, zpos), (tpos, z_up), (tpos, z_dn)):
        pl.semaphore_signal(barrier, inc=1, device_id=target, device_id_type=MESH)

    lane = lax.broadcasted_iota(jnp.int32, (DOF, LANES), 1)
    row = lax.broadcasted_iota(jnp.int32, (DOF, LANES), 0)
    low = lane < HALF
    site = lane % HALF
    x_at = site % 4
    y_at = (site // 4) % 4
    z_at = site // 16
    sign = jnp.where(row < DOF // 2, 1.0, -1.0).astype(f32)
    low8 = low[0:8]
    tail_keep = (low8 & (row[0:8] < 4)) | (jnp.logical_not(low8) & (row[0:8] >= 4))

    def pack(mat, half):
        source = lax.broadcasted_iota(jnp.int32, (2 * LANES, LANES), 0)
        target = lax.broadcasted_iota(jnp.int32, (2 * LANES, LANES), 1)
        wanted = (target // HALF) * LANES + half * HALF + target % HALF
        select = jnp.where(source == wanted, 1.0, 0.0).astype(jnp.bfloat16)
        for out_at, lo_at, hi_at, count in ((0, 0, 8, 8), (8, 16, 24, 8), (16, 32, 36, 4)):
            parts = []
            for comp in range(2):
                upper = raw[mat, comp, lo_at : lo_at + count].reshape(count * DOF, LANES)
                lower = raw[mat, comp, hi_at : hi_at + count].reshape(count * DOF, LANES)
                both_rows = jnp.concatenate([upper, lower], axis=1)
                out = jnp.dot(both_rows, select, preferred_element_type=f32)
                parts.append(out.reshape(count, DOF, LANES))
            mats[half, mat, out_at : out_at + count, 0] = parts[0]
            mats[half, mat, out_at : out_at + count, 1] = parts[1]
            mats[half, mat, out_at : out_at + count, 2] = parts[0] + parts[1]

    def dup(x, half):
        return jnp.where((lane // HALF) == half, x, roll(x, HALF))

    def split_dup(x):
        turned = roll(x, HALF)
        return jnp.where(low, x, turned), jnp.where(low, turned, x)

    z8 = z_at[0:8]

    def face_pack(v):
        tiles = [v[8 * k : 8 * k + 8] for k in range(5)]
        mixed = tiles[0]
        for k in range(1, 4):
            mixed = jnp.where(z8 == k, roll(tiles[k], 16 * k), mixed)
        return jnp.concatenate([mixed, tiles[4]], axis=0)

    def face_unpack(m, slot):
        parts = []
        for k in range(5):
            tile = m[0:8] if k < 4 else m[8:16]
            turn = 16 * (slot - k % 4)
            parts.append((roll(tile, turn), roll(tile, turn + HALF)))
        re = jnp.concatenate([jnp.where(low8, p, q) for p, q in parts], axis=0)
        im = jnp.concatenate([jnp.where(low8, q, p) for p, q in parts], axis=0)
        return jnp.where(z_at == slot, re, 0.0), jnp.where(z_at == slot, im, 0.0)

    def store_bcast(re, im):
        def packed(v):
            tail = v[32:40]
            return jnp.concatenate(
                [
                    jnp.where(low8, v[0:8], v[8:16]),
                    jnp.where(low8, v[16:24], v[24:32]),
                    jnp.where(low8, tail, pltpu.roll(tail, 4, axis=0)),
                ],
                axis=0,
            )

        wr = packed(re * sign)
        wi = packed(im * sign)
        bcast[0, 0:24] = wr
        bcast[1, 0:24] = -(wr + wi)
        bcast[2, 0:24] = wr - wi

    def combos(re, im):
        return re, im - re, re + im

    def forward(i, block, vec, fresh):
        k1 = fold_rows(block[2] * vec[0])
        k2 = fold_rows(block[0] * vec[1])
        k3 = fold_rows(block[1] * vec[2])
        if fresh:
            fwd_re[i] = k1 - k3
            fwd_im[i] = k1 + k2
        else:
            fwd_re[i] = fwd_re[i] + (k1 - k3)
            fwd_im[i] = fwd_im[i] + (k1 + k2)

    def get(half, mat, i):
        return tuple(mats[half, mat, i, k] for k in range(3))

    def forward_only(half, mat, re, im, fresh):
        vec = combos(re, im)

        def one(i, carry):
            forward(i, get(half, mat, i), vec, fresh)
            return carry

        lax.fori_loop(0, PAIRS, one, 0, unroll=20)

    def accumulate(i, block, acc):
        w1 = bcast[0, pl.ds(i, 1), :]
        w2 = bcast[1, pl.ds(i, 1), :]
        w3 = bcast[2, pl.ds(i, 1), :]
        return acc[0] + block[2] * w1, acc[1] + block[0] * w2, acc[2] + block[1] * w3

    def finish(acc):
        return sign * (acc[0] - acc[2]), -sign * (acc[0] + acc[1])

    zeros3 = (jnp.zeros((DOF, LANES), f32),) * 3

    def both(half, mat, re, im):
        vec = combos(re, im)

        def one(i, acc):
            block = get(half, mat, i)
            forward(i, block, vec, False)
            return accumulate(i, block, acc)

        return finish(lax.fori_loop(0, PAIRS, one, zeros3, unroll=20))

    def backward_only(half, mat):
        def one(i, acc):
            return accumulate(i, get(half, mat, i), acc)

        return finish(lax.fori_loop(0, PAIRS, one, zeros3, unroll=20))

    sub = lax.broadcasted_iota(jnp.int32, (8, LANES), 0)

    def pair(lo, hi, width):
        keep = (sub & width) == 0
        return jnp.where(keep, lo, hi) + pltpu.roll(jnp.where(keep, hi, lo), width, axis=0)

    def fold_eight(tiles):
        ones = [pair(tiles[2 * k], tiles[2 * k + 1], 1) for k in range(4)]
        twos = [pair(ones[2 * k], ones[2 * k + 1], 2) for k in range(2)]
        return pair(twos[0], twos[1], 4)

    def gather_forward(ref):
        groups = []
        for start in (0, 8, 16):
            if start < 16:
                rows = fold_eight([ref[start + k] for k in range(8)])
            else:
                rows = fold_eight([ref[start + k % 4] for k in range(8)])
            turned = roll(rows, HALF)
            if start < 16:
                groups.append(jnp.where(low8, rows, turned))
                groups.append(jnp.where(low8, turned, rows))
            else:
                groups.append(jnp.where(tail_keep, rows, turned))
        return jnp.concatenate(groups, axis=0)

    def total(x):
        lanes = jnp.broadcast_to(jnp.sum(fold_rows(x), axis=1, keepdims=True), (8, LANES))
        lanes = lanes + pltpu.roll(lanes, 4, axis=0)
        lanes = lanes + pltpu.roll(lanes, 2, axis=0)
        lanes = lanes + pltpu.roll(lanes, 1, axis=0)
        return 0.5 * lanes

    def spread(x):
        return jnp.concatenate([x] * 5, axis=0)

    def mr_step(half, step):
        sr, si = search[0], search[1]
        store_bcast(sr, si)
        forward_only(half, CLOVER, sr, si, True)

        def ahead(v, mat):
            if mat == ZDIR:
                return jnp.where(z_at == 3, 0.0, -roll(v, -16))
            if mat == YDIR:
                return -jnp.where(y_at == 3, roll(v, 12), roll(v, -4))
            return -jnp.where(x_at == 3, roll(v, 3), roll(v, -1))

        zr, zi = both(half, ZDIR, ahead(sr, ZDIR), ahead(si, ZDIR))
        zr, zi = roll(zr, 16), roll(zi, 16)
        yr, yi = both(half, YDIR, ahead(sr, YDIR), ahead(si, YDIR))
        xr, xi = both(half, XDIR, ahead(sr, XDIR), ahead(si, XDIR))

        def behind(z, y, x):
            y = jnp.where(y_at == 0, roll(y, -12), roll(y, 4))
            x = jnp.where(x_at == 0, roll(x, -3), roll(x, 1))
            out = jnp.where(z_at == 0, 0.0, z) + y + x
            return out + roll(out, HALF)

        qr = gather_forward(fwd_re) - behind(zr, yr, xr)
        qi = gather_forward(fwd_im) - behind(zi, yi, xi)
        nr = total(qr * sr + qi * si)
        ni = total(qr * si - qi * sr)
        inv = 1.0 / (total(qr * qr + qi * qi) + 1e-6)
        live = step < steps_ref[half]
        ar = spread(jnp.where(live, nr * inv, 0.0))
        ai = spread(jnp.where(live, ni * inv, 0.0))
        corr[0] = corr[0] + (ar * sr - ai * si)
        corr[1] = corr[1] + (ar * si + ai * sr)
        face[0] = face[0] + (ar * zr - ai * zi)
        face[1] = face[1] + (ar * zi + ai * zr)
        search[0] = sr - (ar * qr - ai * qi)
        search[1] = si - (ar * qi + ai * qr)

    first_half = lax.rem(zpos, 2)
    rhs_load.wait()
    steps_load.wait()
    for comp in range(2):
        full = rhs_ref[comp]
        for half in range(2):
            resid[half, comp] = dup(full, half)
            solu[half, comp] = jnp.zeros((DOF, LANES), f32)

    for mat in (CLOVER, ZDIR, YDIR, XDIR, TDIR):
        load(mat).wait()
        pack(mat, first_half)

    def copies(turn, t_to):
        t_copy = pltpu.make_async_remote_copy(
            src_ref=tsend.at[turn],
            dst_ref=trecv.at[turn],
            send_sem=send_sem.at[turn, 0],
            recv_sem=recv_sem.at[turn, 0],
            device_id=(t_to, zpos),
            device_id_type=MESH,
        )
        up_copy = pltpu.make_async_remote_copy(
            src_ref=zup_send.at[turn],
            dst_ref=zup_recv.at[turn],
            send_sem=send_sem.at[turn, 1],
            recv_sem=recv_sem.at[turn, 1],
            device_id=(tpos, z_up),
            device_id_type=MESH,
        )
        dn_copy = pltpu.make_async_remote_copy(
            src_ref=zdn_send.at[turn],
            dst_ref=zdn_recv.at[turn],
            send_sem=send_sem.at[turn, 2],
            recv_sem=recv_sem.at[turn, 2],
            device_id=(tpos, z_dn),
            device_id_type=MESH,
        )
        return t_copy, up_copy, dn_copy

    def half_sweep(turn, carry):
        half = lax.rem(turn + zpos, 2)
        other = 1 - half
        t_to = jnp.where(half == 0, t_dn, t_up)
        t_copy, up_copy, dn_copy = copies(turn, t_to)
        for comp in range(2):
            search[comp] = resid[half, comp]
            corr[comp] = jnp.zeros((DOF, LANES), f32)
            face[comp] = jnp.zeros((DOF, LANES), f32)

        def step(k, c):
            mr_step(half, k)
            return c

        lax.fori_loop(0, MR_MAX, step, 0)

        @pl.when(turn == 0)
        def _():
            pl.semaphore_wait(barrier, 4)

        er, ei = corr[0], corr[1]

        @pl.when(half == 0)
        def _():
            tsend[turn] = jnp.where(low, er, ei)
            t_copy.start()

        zdn_send[turn] = face_pack(jnp.where(low, er, ei))
        fr, fi = face[0], face[1]
        fr = fr + roll(fr, HALF)
        fi = fi + roll(fi, HALF)
        zup_send[turn] = face_pack(jnp.where(low, fr, fi))
        dn_copy.start()
        up_copy.start()
        store_bcast(er, ei)
        pr, pi = backward_only(half, TDIR)
        pr = pr + roll(pr, HALF)
        pi = pi + roll(pi, HALF)

        @pl.when(half == 1)
        def _():
            tsend[turn] = jnp.where(low, pr, pi)
            t_copy.start()

        for comp in range(2):
            resid[half, comp] = search[comp]
            solu[half, comp] = solu[half, comp] + corr[comp]
        face[0] = pr
        face[1] = pi

        @pl.when(turn == 0)
        def _():
            for mat in (TDIR, ZDIR, CLOVER, YDIR, XDIR):
                pack(mat, other)

        dn_copy.wait_recv()
        zr, zi = face_unpack(zdn_recv[turn], 3)
        forward_only(other, ZDIR, zr, zi, True)

        @pl.when(half == 1)
        def _():
            forward_only(other, TDIR, corr[0], corr[1], False)

        up_copy.wait_recv()
        ur, ui = face_unpack(zup_recv[turn], 0)
        ur = ur + resid[other, 0]
        ui = ui + resid[other, 1]

        @pl.when(half == 1)
        def _():
            resid[other, 0] = ur + gather_forward(fwd_re)
            resid[other, 1] = ui + gather_forward(fwd_im)

        @pl.when(half == 0)
        def _():
            resid[other, 0] = ur + face[0]
            resid[other, 1] = ui + face[1]

        t_copy.wait_recv()
        tr, ti = split_dup(trecv[turn])

        @pl.when(half == 0)
        def _():
            forward_only(other, TDIR, tr, ti, False)
            resid[other, 0] = resid[other, 0] + gather_forward(fwd_re)
            resid[other, 1] = resid[other, 1] + gather_forward(fwd_im)

        @pl.when(half == 1)
        def _():
            resid[other, 0] = resid[other, 0] + tr
            resid[other, 1] = resid[other, 1] + ti

        return carry

    lax.fori_loop(0, HALF_SWEEPS, half_sweep, 0)

    for comp in range(2):
        sol_ref[comp] = jnp.where(low, solu[0, comp], solu[1, comp])
        res_ref[comp] = jnp.where(low, resid[0, comp], resid[1, comp])

    def drain(turn, carry):
        for copy in copies(turn, t_up):
            copy.wait_send()
        return carry

    lax.fori_loop(0, HALF_SWEEPS, drain, 0)


def solution(mesh):
    time_count, space_count = mesh.shape["ta"], mesh.shape["sa"]
    f32 = jnp.float32
    vmem = pltpu.VMEM
    field = (2, DOF, LANES)

    def shards(rhs, links, clover, mr_steps):
        out = jax.ShapeDtypeStruct(field, f32)
        message = vmem((HALF_SWEEPS, DOF, LANES), f32)
        small = vmem((HALF_SWEEPS, 16, LANES), f32)
        sol, res = pl.pallas_call(
            functools.partial(kernel, time_count, space_count),
            out_shape=(out, out),
            in_specs=[
                pl.BlockSpec(memory_space=pltpu.HBM),
                pl.BlockSpec(memory_space=pltpu.HBM),
                pl.BlockSpec(memory_space=pltpu.HBM),
                pl.BlockSpec(memory_space=pltpu.HBM),
            ],
            out_specs=(pl.BlockSpec(memory_space=pltpu.VMEM),) * 2,
            scratch_shapes=[
                vmem((2, 5, PAIRS, 3, DOF, LANES), f32),
                vmem((5, 2, DOF, DOF, LANES), jnp.bfloat16),
                vmem((2,) + field, f32),
                vmem((2,) + field, f32),
                vmem((8, DOF, LANES), f32),
                vmem((3, 32, LANES), f32),
                vmem((PAIRS, 8, LANES), f32),
                vmem((PAIRS, 8, LANES), f32),
                message,
                small,
                small,
                message,
                small,
                small,
                pltpu.SMEM((2,), jnp.int32),
                pltpu.SemaphoreType.DMA((7,)),
                pltpu.SemaphoreType.DMA((HALF_SWEEPS, 3)),
                pltpu.SemaphoreType.DMA((HALF_SWEEPS, 3)),
            ],
            compiler_params=pltpu.CompilerParams(
                collective_id=0, has_side_effects=True, vmem_limit_bytes=40 * 2**20
            ),
        )(
            pltpu.with_memory_space_constraint(rhs.reshape(field), pltpu.HBM),
            pltpu.with_memory_space_constraint(links.reshape(4, 2, DOF, DOF, LANES), pltpu.HBM),
            pltpu.with_memory_space_constraint(clover.reshape(2, DOF, DOF, LANES), pltpu.HBM),
            pltpu.with_memory_space_constraint(mr_steps.reshape(2), pltpu.HBM),
        )
        shape = rhs.shape
        return sol.reshape(shape), res.reshape(shape)

    placed = (
        P(None, None, None, "ta", "sa", None),
        P(None, None, None, None, "ta", "sa", None),
        P(None, None, None, "ta", "sa", None),
        P("ta", "sa", None),
    )
    return jax.shard_map(
        shards,
        mesh=mesh,
        in_specs=placed,
        out_specs=(P(None, None, None, "ta", "sa", None),) * 2,
        check_vma=False,
    )
```

```python
import functools

import jax
import jax.numpy as jnp
from jax import lax
from jax.experimental import pallas as pl
from jax.experimental.pallas import tpu as pltpu
from jax.sharding import PartitionSpec as P

MESH = pl.DeviceIdType.MESH
MR_MAX = 3
HALF_SWEEPS = 4
DOF = 40
PAIRS = 20
LANES = 128
HALF = 64
CLOVER, ZDIR, YDIR, XDIR, TDIR = 0, 1, 2, 3, 4
LINK_OF = {TDIR: 0, ZDIR: 1, YDIR: 2, XDIR: 3}


def roll(x, amount):
    return pltpu.roll(x, amount % LANES, axis=1)


def fold_rows(x):
    return x[0:8] + x[8:16] + x[16:24] + x[24:32] + x[32:40]


def kernel(
    time_count,
    space_count,
    rhs_hbm,
    links_ref,
    clover_ref,
    steps_hbm,
    sol_ref,
    res_ref,
    mats,
    raw,
    resid,
    solu,
    state,
    bcast,
    fwd_re,
    fwd_im,
    tsend,
    zup_send,
    zdn_send,
    trecv,
    zup_recv,
    zdn_recv,
    esend,
    erecv,
    asend,
    arecv,
    steps_ref,
    load_sem,
    send_sem,
    recv_sem,
):
    f32 = jnp.float32
    search, corr, face, rhs_ref = (state.at[pl.ds(2 * k, 2)] for k in range(4))
    tpos = lax.axis_index("ta")
    zpos = lax.axis_index("sa")
    t_up = lax.rem(tpos + 1, time_count)
    t_dn = lax.rem(tpos + time_count - 1, time_count)
    z_up = lax.rem(zpos + 1, space_count)
    z_dn = lax.rem(zpos + space_count - 1, space_count)

    def load(mat):
        source = clover_ref if mat == CLOVER else links_ref.at[LINK_OF[mat]]
        return pltpu.make_async_copy(source, raw.at[mat], load_sem.at[mat])

    rhs_load = pltpu.make_async_copy(rhs_hbm, rhs_ref, load_sem.at[5])
    rhs_load.start()
    steps_load = pltpu.make_async_copy(steps_hbm, steps_ref, load_sem.at[6])
    steps_load.start()
    for mat in (CLOVER, ZDIR, YDIR, XDIR, TDIR):
        load(mat).start()
    barrier = pltpu.get_barrier_semaphore()
    for target in ((t_up, zpos), (t_dn, zpos), (tpos, z_up), (tpos, z_dn)):
        pl.semaphore_signal(barrier, inc=1, device_id=target, device_id_type=MESH)

    lane = lax.broadcasted_iota(jnp.int32, (DOF, LANES), 1)
    row = lax.broadcasted_iota(jnp.int32, (DOF, LANES), 0)
    low = lane < HALF
    site = lane % HALF
    x_at = site % 4
    y_at = (site // 4) % 4
    z_at = site // 16
    sign = jnp.where(row < DOF // 2, 1.0, -1.0).astype(f32)
    low8 = low[0:8]
    tail_keep = (low8 & (row[0:8] < 4)) | (jnp.logical_not(low8) & (row[0:8] >= 4))

    def pack(mat, half):
        source = lax.broadcasted_iota(jnp.int32, (2 * LANES, LANES), 0)
        target = lax.broadcasted_iota(jnp.int32, (2 * LANES, LANES), 1)
        wanted = (target // HALF) * LANES + half * HALF + target % HALF
        select = jnp.where(source == wanted, 1.0, 0.0).astype(jnp.bfloat16)
        for out_at, lo_at, hi_at, count in ((0, 0, 8, 8), (8, 16, 24, 8), (16, 32, 36, 4)):
            parts = []
            for comp in range(2):
                upper = raw[mat, comp, lo_at : lo_at + count].reshape(count * DOF, LANES)
                lower = raw[mat, comp, hi_at : hi_at + count].reshape(count * DOF, LANES)
                both_rows = jnp.concatenate([upper, lower], axis=1)
                out = jnp.dot(both_rows, select, preferred_element_type=f32)
                parts.append(out.reshape(count, DOF, LANES))
            mats[half, mat, out_at : out_at + count, 0] = parts[0]
            mats[half, mat, out_at : out_at + count, 1] = parts[1]
            mats[half, mat, out_at : out_at + count, 2] = parts[0] + parts[1]

    def dup(x, half):
        return jnp.where((lane // HALF) == half, x, roll(x, HALF))

    def split_dup(x):
        turned = roll(x, HALF)
        return jnp.where(low, x, turned), jnp.where(low, turned, x)

    z8 = z_at[0:8]

    def face_pack(v):
        tiles = [v[8 * k : 8 * k + 8] for k in range(5)]
        mixed = tiles[0]
        for k in range(1, 4):
            mixed = jnp.where(z8 == k, roll(tiles[k], 16 * k), mixed)
        return jnp.concatenate([mixed, tiles[4]], axis=0)

    def face_unpack(m, slot):
        parts = []
        for k in range(5):
            tile = m[0:8] if k < 4 else m[8:16]
            turn = 16 * (slot - k % 4)
            parts.append((roll(tile, turn), roll(tile, turn + HALF)))
        re = jnp.concatenate([jnp.where(low8, p, q) for p, q in parts], axis=0)
        im = jnp.concatenate([jnp.where(low8, q, p) for p, q in parts], axis=0)
        return jnp.where(z_at == slot, re, 0.0), jnp.where(z_at == slot, im, 0.0)

    def store_bcast(re, im):
        def packed(v):
            tail = v[32:40]
            return jnp.concatenate(
                [
                    jnp.where(low8, v[0:8], v[8:16]),
                    jnp.where(low8, v[16:24], v[24:32]),
                    jnp.where(low8, tail, pltpu.roll(tail, 4, axis=0)),
                ],
                axis=0,
            )

        wr = packed(re * sign)
        wi = packed(im * sign)
        bcast[0, 0:24] = wr
        bcast[1, 0:24] = -(wr + wi)
        bcast[2, 0:24] = wr - wi

    def combos(re, im):
        return re, im - re, re + im

    def forward(i, block, vec, fresh):
        k1 = fold_rows(block[2] * vec[0])
        k2 = fold_rows(block[0] * vec[1])
        k3 = fold_rows(block[1] * vec[2])
        if fresh:
            fwd_re[i] = k1 - k3
            fwd_im[i] = k1 + k2
        else:
            fwd_re[i] = fwd_re[i] + (k1 - k3)
            fwd_im[i] = fwd_im[i] + (k1 + k2)

    def get(half, mat, i):
        return tuple(mats[half, mat, i, k] for k in range(3))

    def forward_only(half, mat, re, im, fresh):
        vec = combos(re, im)

        def one(i, carry):
            forward(i, get(half, mat, i), vec, fresh)
            return carry

        lax.fori_loop(0, PAIRS, one, 0, unroll=20)

    def accumulate(i, block, acc):
        w1 = bcast[0, pl.ds(i, 1), :]
        w2 = bcast[1, pl.ds(i, 1), :]
        w3 = bcast[2, pl.ds(i, 1), :]
        return acc[0] + block[2] * w1, acc[1] + block[0] * w2, acc[2] + block[1] * w3

    def finish(acc):
        return sign * (acc[0] - acc[2]), -sign * (acc[0] + acc[1])

    zeros3 = (jnp.zeros((DOF, LANES), f32),) * 3

    def both(half, mat, re, im):
        vec = combos(re, im)

        def one(i, acc):
            block = get(half, mat, i)
            forward(i, block, vec, False)
            return accumulate(i, block, acc)

        return finish(lax.fori_loop(0, PAIRS, one, zeros3, unroll=20))

    def backward_only(half, mat):
        def one(i, acc):
            return accumulate(i, get(half, mat, i), acc)

        return finish(lax.fori_loop(0, PAIRS, one, zeros3, unroll=20))

    sub = lax.broadcasted_iota(jnp.int32, (8, LANES), 0)

    def pair(lo, hi, width):
        keep = (sub & width) == 0
        return jnp.where(keep, lo, hi) + pltpu.roll(jnp.where(keep, hi, lo), width, axis=0)

    def fold_eight(tiles):
        ones = [pair(tiles[2 * k], tiles[2 * k + 1], 1) for k in range(4)]
        twos = [pair(ones[2 * k], ones[2 * k + 1], 2) for k in range(2)]
        return pair(twos[0], twos[1], 4)

    def gather_forward(ref):
        groups = []
        for start in (0, 8, 16):
            if start < 16:
                rows = fold_eight([ref[start + k] for k in range(8)])
            else:
                rows = fold_eight([ref[start + k % 4] for k in range(8)])
            turned = roll(rows, HALF)
            if start < 16:
                groups.append(jnp.where(low8, rows, turned))
                groups.append(jnp.where(low8, turned, rows))
            else:
                groups.append(jnp.where(tail_keep, rows, turned))
        return jnp.concatenate(groups, axis=0)

    def total(x):
        lanes = jnp.broadcast_to(jnp.sum(fold_rows(x), axis=1, keepdims=True), (8, LANES))
        lanes = lanes + pltpu.roll(lanes, 4, axis=0)
        lanes = lanes + pltpu.roll(lanes, 2, axis=0)
        lanes = lanes + pltpu.roll(lanes, 1, axis=0)
        return 0.5 * lanes

    def spread(x):
        return jnp.concatenate([x] * 5, axis=0)

    def mr_step(half, step):
        sr, si = search[0], search[1]
        store_bcast(sr, si)
        forward_only(half, CLOVER, sr, si, True)

        def ahead(v, mat):
            if mat == ZDIR:
                return jnp.where(z_at == 3, 0.0, -roll(v, -16))
            if mat == YDIR:
                return -jnp.where(y_at == 3, roll(v, 12), roll(v, -4))
            return -jnp.where(x_at == 3, roll(v, 3), roll(v, -1))

        zr, zi = both(half, ZDIR, ahead(sr, ZDIR), ahead(si, ZDIR))
        zr, zi = roll(zr, 16), roll(zi, 16)
        yr, yi = both(half, YDIR, ahead(sr, YDIR), ahead(si, YDIR))
        xr, xi = both(half, XDIR, ahead(sr, XDIR), ahead(si, XDIR))

        def behind(z, y, x):
            y = jnp.where(y_at == 0, roll(y, -12), roll(y, 4))
            x = jnp.where(x_at == 0, roll(x, -3), roll(x, 1))
            out = jnp.where(z_at == 0, 0.0, z) + y + x
            return out + roll(out, HALF)

        qr = gather_forward(fwd_re) - behind(zr, yr, xr)
        qi = gather_forward(fwd_im) - behind(zi, yi, xi)
        nr = total(qr * sr + qi * si)
        ni = total(qr * si - qi * sr)
        inv = 1.0 / (total(qr * qr + qi * qi) + 1e-6)
        live = step < steps_ref[half]
        ar8 = jnp.where(live, nr * inv, 0.0)
        ai8 = jnp.where(live, ni * inv, 0.0)
        ar, ai = spread(ar8), spread(ai8)
        corr[0] = corr[0] + (ar * sr - ai * si)
        corr[1] = corr[1] + (ar * si + ai * sr)
        face[0] = face[0] + (ar * zr - ai * zi)
        face[1] = face[1] + (ar * zi + ai * zr)
        search[0] = sr - (ar * qr - ai * qi)
        search[1] = si - (ar * qi + ai * qr)
        return ar8, ai8

    first_half = lax.rem(zpos, 2)
    rhs_load.wait()
    steps_load.wait()
    for comp in range(2):
        full = rhs_ref[comp]
        for half in range(2):
            resid[half, comp] = dup(full, half)
            solu[half, comp] = jnp.zeros((DOF, LANES), f32)

    for mat in (CLOVER, ZDIR, YDIR, XDIR, TDIR):
        load(mat).wait()
        pack(mat, first_half)

    def copies(turn):
        t_copy = pltpu.make_async_remote_copy(
            src_ref=tsend.at[turn],
            dst_ref=trecv.at[turn],
            send_sem=send_sem.at[turn, 0],
            recv_sem=recv_sem.at[turn, 0],
            device_id=(t_up, zpos),
            device_id_type=MESH,
        )
        up_copy = pltpu.make_async_remote_copy(
            src_ref=zup_send.at[turn],
            dst_ref=zup_recv.at[turn],
            send_sem=send_sem.at[turn, 1],
            recv_sem=recv_sem.at[turn, 1],
            device_id=(tpos, z_up),
            device_id_type=MESH,
        )
        dn_copy = pltpu.make_async_remote_copy(
            src_ref=zdn_send.at[turn],
            dst_ref=zdn_recv.at[turn],
            send_sem=send_sem.at[turn, 2],
            recv_sem=recv_sem.at[turn, 2],
            device_id=(tpos, z_dn),
            device_id_type=MESH,
        )
        early_copy = pltpu.make_async_remote_copy(
            src_ref=esend.at[turn],
            dst_ref=erecv.at[turn],
            send_sem=send_sem.at[turn, 3],
            recv_sem=recv_sem.at[turn, 3],
            device_id=(t_dn, zpos),
            device_id_type=MESH,
        )
        alpha_copy = pltpu.make_async_remote_copy(
            src_ref=asend.at[turn],
            dst_ref=arecv.at[turn],
            send_sem=send_sem.at[turn, 4],
            recv_sem=recv_sem.at[turn, 4],
            device_id=(t_dn, zpos),
            device_id_type=MESH,
        )
        return t_copy, up_copy, dn_copy, early_copy, alpha_copy

    def half_sweep(turn, carry):
        half = lax.rem(turn + zpos, 2)
        other = 1 - half
        t_copy, up_copy, dn_copy, early_copy, alpha_copy = copies(turn)
        for comp in range(2):
            search[comp] = resid[half, comp]
            corr[comp] = jnp.zeros((DOF, LANES), f32)
            face[comp] = jnp.zeros((DOF, LANES), f32)

        def step(k, c):
            mr_step(half, k)
            return c

        lax.fori_loop(0, MR_MAX - 1, step, 0, unroll=True)

        @pl.when(turn == 0)
        def _():
            pl.semaphore_wait(barrier, 4)

        @pl.when(half == 0)
        def _():
            esend[turn, 0] = jnp.where(low, corr[0], corr[1])
            esend[turn, 1] = jnp.where(low, search[0], search[1])
            early_copy.start()

        ar8, ai8 = mr_step(half, MR_MAX - 1)
        er, ei = corr[0], corr[1]

        @pl.when(half == 0)
        def _():
            asend[turn] = jnp.where(sub < 4, ar8, ai8)
            alpha_copy.start()

        zdn_send[turn] = face_pack(jnp.where(low, er, ei))
        fr, fi = face[0], face[1]
        fr = fr + roll(fr, HALF)
        fi = fi + roll(fi, HALF)
        zup_send[turn] = face_pack(jnp.where(low, fr, fi))
        dn_copy.start()
        up_copy.start()
        store_bcast(er, ei)
        pr, pi = backward_only(half, TDIR)
        pr = pr + roll(pr, HALF)
        pi = pi + roll(pi, HALF)

        @pl.when(half == 1)
        def _():
            tsend[turn] = jnp.where(low, pr, pi)
            t_copy.start()

        for comp in range(2):
            resid[half, comp] = search[comp]
            solu[half, comp] = solu[half, comp] + corr[comp]
        face[0] = pr
        face[1] = pi

        @pl.when(turn == 0)
        def _():
            for mat in (TDIR, ZDIR, CLOVER, YDIR, XDIR):
                pack(mat, other)

        dn_copy.wait_recv()
        zr, zi = face_unpack(zdn_recv[turn], 3)
        forward_only(other, ZDIR, zr, zi, True)

        @pl.when(half == 1)
        def _():
            forward_only(other, TDIR, corr[0], corr[1], False)

        up_copy.wait_recv()
        ur, ui = face_unpack(zup_recv[turn], 0)
        ur = ur + resid[other, 0]
        ui = ui + resid[other, 1]

        @pl.when(half == 1)
        def _():
            resid[other, 0] = ur + gather_forward(fwd_re)
            resid[other, 1] = ui + gather_forward(fwd_im)

        @pl.when(half == 0)
        def _():
            early_copy.wait_recv()
            tr, ti = split_dup(erecv[turn, 0])
            forward_only(other, TDIR, tr, ti, False)
            br = ur + face[0] + gather_forward(fwd_re)
            bi = ui + face[1] + gather_forward(fwd_im)
            tr, ti = split_dup(erecv[turn, 1])
            forward_only(other, TDIR, tr, ti, True)
            gr = gather_forward(fwd_re)
            gi = gather_forward(fwd_im)
            alpha_copy.wait_recv()
            got = arecv[turn]
            swapped = pltpu.roll(got, 4, axis=0)
            cr = spread(jnp.where(sub < 4, got, swapped))
            ci = spread(jnp.where(sub < 4, swapped, got))
            resid[other, 0] = br + (cr * gr - ci * gi)
            resid[other, 1] = bi + (cr * gi + ci * gr)

        @pl.when(half == 1)
        def _():
            t_copy.wait_recv()
            tr, ti = split_dup(trecv[turn])
            resid[other, 0] = resid[other, 0] + tr
            resid[other, 1] = resid[other, 1] + ti

        return carry

    lax.fori_loop(0, HALF_SWEEPS, half_sweep, 0)

    for comp in range(2):
        sol_ref[comp] = jnp.where(low, solu[0, comp], solu[1, comp])
        res_ref[comp] = jnp.where(low, resid[0, comp], resid[1, comp])

    def drain(turn, carry):
        half = lax.rem(turn + zpos, 2)
        t_copy, up_copy, dn_copy, early_copy, alpha_copy = copies(turn)
        up_copy.wait_send()
        dn_copy.wait_send()

        @pl.when(half == 0)
        def _():
            early_copy.wait_send()
            alpha_copy.wait_send()

        @pl.when(half == 1)
        def _():
            t_copy.wait_send()

        return carry

    lax.fori_loop(0, HALF_SWEEPS, drain, 0)


def solution(mesh):
    time_count, space_count = mesh.shape["ta"], mesh.shape["sa"]
    f32 = jnp.float32
    vmem = pltpu.VMEM
    field = (2, DOF, LANES)

    def shards(rhs, links, clover, mr_steps):
        out = jax.ShapeDtypeStruct(field, f32)
        message = vmem((HALF_SWEEPS, DOF, LANES), f32)
        small = vmem((HALF_SWEEPS, 16, LANES), f32)
        sol, res = pl.pallas_call(
            functools.partial(kernel, time_count, space_count),
            out_shape=(out, out),
            in_specs=[
                pl.BlockSpec(memory_space=pltpu.HBM),
                pl.BlockSpec(memory_space=pltpu.HBM),
                pl.BlockSpec(memory_space=pltpu.HBM),
                pl.BlockSpec(memory_space=pltpu.HBM),
            ],
            out_specs=(pl.BlockSpec(memory_space=pltpu.VMEM),) * 2,
            scratch_shapes=[
                vmem((2, 5, PAIRS, 3, DOF, LANES), f32),
                vmem((5, 2, DOF, DOF, LANES), jnp.bfloat16),
                vmem((2,) + field, f32),
                vmem((2,) + field, f32),
                vmem((8, DOF, LANES), f32),
                vmem((3, 32, LANES), f32),
                vmem((PAIRS, 8, LANES), f32),
                vmem((PAIRS, 8, LANES), f32),
                message,
                small,
                small,
                message,
                small,
                small,
                vmem((HALF_SWEEPS, 2, DOF, LANES), f32),
                vmem((HALF_SWEEPS, 2, DOF, LANES), f32),
                vmem((HALF_SWEEPS, 8, LANES), f32),
                vmem((HALF_SWEEPS, 8, LANES), f32),
                pltpu.SMEM((2,), jnp.int32),
                pltpu.SemaphoreType.DMA((7,)),
                pltpu.SemaphoreType.DMA((HALF_SWEEPS, 5)),
                pltpu.SemaphoreType.DMA((HALF_SWEEPS, 5)),
            ],
            compiler_params=pltpu.CompilerParams(
                collective_id=0, has_side_effects=True, vmem_limit_bytes=40 * 2**20
            ),
        )(
            pltpu.with_memory_space_constraint(rhs.reshape(field), pltpu.HBM),
            pltpu.with_memory_space_constraint(links.reshape(4, 2, DOF, DOF, LANES), pltpu.HBM),
            pltpu.with_memory_space_constraint(clover.reshape(2, DOF, DOF, LANES), pltpu.HBM),
            pltpu.with_memory_space_constraint(mr_steps.reshape(2), pltpu.HBM),
        )
        shape = rhs.shape
        return sol.reshape(shape), res.reshape(shape)

    placed = (
        P(None, None, None, "ta", "sa", None),
        P(None, None, None, None, "ta", "sa", None),
        P(None, None, None, "ta", "sa", None),
        P("ta", "sa", None),
    )
    return jax.shard_map(
        shards,
        mesh=mesh,
        in_specs=placed,
        out_specs=(P(None, None, None, "ta", "sa", None),) * 2,
        check_vma=False,
    )
```

```python
import functools

import jax
import jax.numpy as jnp
from jax import lax
from jax.experimental import pallas as pl
from jax.experimental.pallas import tpu as pltpu
from jax.sharding import PartitionSpec as P

MESH = pl.DeviceIdType.MESH
MR_MAX = 3
HALF_SWEEPS = 4
DOF = 40
PAIRS = 20
LANES = 128
HALF = 64
CLOVER, ZDIR, YDIR, XDIR, TDIR = 0, 1, 2, 3, 4
LINK_OF = {TDIR: 0, ZDIR: 1, YDIR: 2, XDIR: 3}


def roll(x, amount):
    return pltpu.roll(x, amount % LANES, axis=1)


def fold_rows(x):
    return x[0:8] + x[8:16] + x[16:24] + x[24:32] + x[32:40]


def kernel(
    time_count,
    space_count,
    rhs_hbm,
    links_ref,
    clover_ref,
    steps_hbm,
    sol_ref,
    res_ref,
    mats,
    raw,
    resid,
    solu,
    state,
    bcast,
    fwd_re,
    fwd_im,
    tsend,
    zup_send,
    zdn_send,
    trecv,
    zup_recv,
    zdn_recv,
    steps_ref,
    load_sem,
    send_sem,
    recv_sem,
):
    f32 = jnp.float32
    search, corr, face, rhs_ref = (state.at[pl.ds(2 * k, 2)] for k in range(4))
    tpos = lax.axis_index("ta")
    zpos = lax.axis_index("sa")
    t_up = lax.rem(tpos + 1, time_count)
    t_dn = lax.rem(tpos + time_count - 1, time_count)
    z_up = lax.rem(zpos + 1, space_count)
    z_dn = lax.rem(zpos + space_count - 1, space_count)

    def load(mat):
        source = clover_ref if mat == CLOVER else links_ref.at[LINK_OF[mat]]
        return pltpu.make_async_copy(source, raw.at[mat], load_sem.at[mat])

    rhs_load = pltpu.make_async_copy(rhs_hbm, rhs_ref, load_sem.at[5])
    rhs_load.start()
    steps_load = pltpu.make_async_copy(steps_hbm, steps_ref, load_sem.at[6])
    steps_load.start()
    for mat in (CLOVER, ZDIR, YDIR, XDIR, TDIR):
        load(mat).start()
    barrier = pltpu.get_barrier_semaphore()
    for target in ((t_up, zpos), (t_dn, zpos), (tpos, z_up), (tpos, z_dn)):
        pl.semaphore_signal(barrier, inc=1, device_id=target, device_id_type=MESH)

    lane = lax.broadcasted_iota(jnp.int32, (DOF, LANES), 1)
    row = lax.broadcasted_iota(jnp.int32, (DOF, LANES), 0)
    low = lane < HALF
    site = lane % HALF
    x_at = site % 4
    y_at = (site // 4) % 4
    z_at = site // 16
    sign = jnp.where(row < DOF // 2, 1.0, -1.0).astype(f32)
    low8 = low[0:8]
    tail_keep = (low8 & (row[0:8] < 4)) | (jnp.logical_not(low8) & (row[0:8] >= 4))

    def pack(mat):
        source = lax.broadcasted_iota(jnp.int32, (2 * LANES, 2 * LANES), 0)
        target = lax.broadcasted_iota(jnp.int32, (2 * LANES, 2 * LANES), 1)
        wanted = (target // HALF % 2) * LANES + target // LANES * HALF + target % HALF
        select = jnp.where(source == wanted, 1.0, 0.0).astype(jnp.bfloat16)
        for out_at, lo_at, hi_at, count in ((0, 0, 8, 8), (8, 16, 24, 8), (16, 32, 36, 4)):
            parts = []
            for comp in range(2):
                upper = raw[mat, comp, lo_at : lo_at + count].reshape(count * DOF, LANES)
                lower = raw[mat, comp, hi_at : hi_at + count].reshape(count * DOF, LANES)
                both_rows = jnp.concatenate([upper, lower], axis=1)
                parts.append(jnp.dot(both_rows, select, preferred_element_type=f32))
            for half in range(2):
                re, im = (p[:, LANES * half : LANES * half + LANES].reshape(count, DOF, LANES) for p in parts)
                mats[half, mat, out_at : out_at + count, 0] = re
                mats[half, mat, out_at : out_at + count, 1] = im
                mats[half, mat, out_at : out_at + count, 2] = re + im

    def dup(x, half):
        return jnp.where((lane // HALF) == half, x, roll(x, HALF))

    def split_dup(x):
        turned = roll(x, HALF)
        return jnp.where(low, x, turned), jnp.where(low, turned, x)

    z8 = z_at[0:8]

    def face_pack(v):
        tiles = [v[8 * k : 8 * k + 8] for k in range(5)]
        mixed = tiles[0]
        for k in range(1, 4):
            mixed = jnp.where(z8 == k, roll(tiles[k], 16 * k), mixed)
        return jnp.concatenate([mixed, tiles[4]], axis=0)

    def face_unpack(m, slot):
        parts = []
        for k in range(5):
            tile = m[0:8] if k < 4 else m[8:16]
            turn = 16 * (slot - k % 4)
            parts.append((roll(tile, turn), roll(tile, turn + HALF)))
        re = jnp.concatenate([jnp.where(low8, p, q) for p, q in parts], axis=0)
        im = jnp.concatenate([jnp.where(low8, q, p) for p, q in parts], axis=0)
        return jnp.where(z_at == slot, re, 0.0), jnp.where(z_at == slot, im, 0.0)

    def store_bcast(re, im):
        def packed(v):
            tail = v[32:40]
            return jnp.concatenate(
                [
                    jnp.where(low8, v[0:8], v[8:16]),
                    jnp.where(low8, v[16:24], v[24:32]),
                    jnp.where(low8, tail, pltpu.roll(tail, 4, axis=0)),
                ],
                axis=0,
            )

        wr = packed(re * sign)
        wi = packed(im * sign)
        bcast[0, 0:24] = wr
        bcast[1, 0:24] = -(wr + wi)
        bcast[2, 0:24] = wr - wi

    def combos(re, im):
        return re, im - re, re + im

    def forward(i, block, vec, fresh):
        k1 = fold_rows(block[2] * vec[0])
        k2 = fold_rows(block[0] * vec[1])
        k3 = fold_rows(block[1] * vec[2])
        if fresh:
            fwd_re[i] = k1 - k3
            fwd_im[i] = k1 + k2
        else:
            fwd_re[i] = fwd_re[i] + (k1 - k3)
            fwd_im[i] = fwd_im[i] + (k1 + k2)

    def get(half, mat, i):
        return tuple(mats[half, mat, i, k] for k in range(3))

    def forward_only(half, mat, re, im, fresh):
        vec = combos(re, im)

        def one(i, carry):
            forward(i, get(half, mat, i), vec, fresh)
            return carry

        lax.fori_loop(0, PAIRS, one, 0, unroll=20)

    def accumulate(i, block, acc):
        w1 = bcast[0, pl.ds(i, 1), :]
        w2 = bcast[1, pl.ds(i, 1), :]
        w3 = bcast[2, pl.ds(i, 1), :]
        return acc[0] + block[2] * w1, acc[1] + block[0] * w2, acc[2] + block[1] * w3

    def finish(acc):
        return sign * (acc[0] - acc[2]), -sign * (acc[0] + acc[1])

    zeros3 = (jnp.zeros((DOF, LANES), f32),) * 3

    def both(half, mat, re, im):
        vec = combos(re, im)

        def one(i, acc):
            block = get(half, mat, i)
            forward(i, block, vec, False)
            return accumulate(i, block, acc)

        return finish(lax.fori_loop(0, PAIRS, one, zeros3, unroll=20))

    def backward_only(half, mat):
        def one(i, acc):
            return accumulate(i, get(half, mat, i), acc)

        return finish(lax.fori_loop(0, PAIRS, one, zeros3, unroll=20))

    sub = lax.broadcasted_iota(jnp.int32, (8, LANES), 0)

    def pair(lo, hi, width):
        keep = (sub & width) == 0
        return jnp.where(keep, lo, hi) + pltpu.roll(jnp.where(keep, hi, lo), width, axis=0)

    def fold_eight(tiles):
        ones = [pair(tiles[2 * k], tiles[2 * k + 1], 1) for k in range(4)]
        twos = [pair(ones[2 * k], ones[2 * k + 1], 2) for k in range(2)]
        return pair(twos[0], twos[1], 4)

    def gather_forward(ref):
        groups = []
        for start in (0, 8, 16):
            if start < 16:
                rows = fold_eight([ref[start + k] for k in range(8)])
            else:
                rows = fold_eight([ref[start + k % 4] for k in range(8)])
            turned = roll(rows, HALF)
            if start < 16:
                groups.append(jnp.where(low8, rows, turned))
                groups.append(jnp.where(low8, turned, rows))
            else:
                groups.append(jnp.where(tail_keep, rows, turned))
        return jnp.concatenate(groups, axis=0)

    def total(x):
        lanes = jnp.broadcast_to(jnp.sum(fold_rows(x), axis=1, keepdims=True), (8, LANES))
        lanes = lanes + pltpu.roll(lanes, 4, axis=0)
        lanes = lanes + pltpu.roll(lanes, 2, axis=0)
        lanes = lanes + pltpu.roll(lanes, 1, axis=0)
        return 0.5 * lanes

    def spread(x):
        return jnp.concatenate([x] * 5, axis=0)

    def mr_step(half, step):
        sr, si = search[0], search[1]
        store_bcast(sr, si)
        forward_only(half, CLOVER, sr, si, True)

        def ahead(v, mat):
            if mat == ZDIR:
                return jnp.where(z_at == 3, 0.0, -roll(v, -16))
            if mat == YDIR:
                return -jnp.where(y_at == 3, roll(v, 12), roll(v, -4))
            return -jnp.where(x_at == 3, roll(v, 3), roll(v, -1))

        zr, zi = both(half, ZDIR, ahead(sr, ZDIR), ahead(si, ZDIR))
        zr, zi = roll(zr, 16), roll(zi, 16)
        yr, yi = both(half, YDIR, ahead(sr, YDIR), ahead(si, YDIR))
        xr, xi = both(half, XDIR, ahead(sr, XDIR), ahead(si, XDIR))

        def behind(z, y, x):
            y = jnp.where(y_at == 0, roll(y, -12), roll(y, 4))
            x = jnp.where(x_at == 0, roll(x, -3), roll(x, 1))
            out = jnp.where(z_at == 0, 0.0, z) + y + x
            return out + roll(out, HALF)

        qr = gather_forward(fwd_re) - behind(zr, yr, xr)
        qi = gather_forward(fwd_im) - behind(zi, yi, xi)
        nr = total(qr * sr + qi * si)
        ni = total(qr * si - qi * sr)
        inv = 1.0 / (total(qr * qr + qi * qi) + 1e-6)
        live = step < steps_ref[half]
        ar = spread(jnp.where(live, nr * inv, 0.0))
        ai = spread(jnp.where(live, ni * inv, 0.0))
        corr[0] = corr[0] + (ar * sr - ai * si)
        corr[1] = corr[1] + (ar * si + ai * sr)
        face[0] = face[0] + (ar * zr - ai * zi)
        face[1] = face[1] + (ar * zi + ai * zr)
        search[0] = sr - (ar * qr - ai * qi)
        search[1] = si - (ar * qi + ai * qr)

    rhs_load.wait()
    steps_load.wait()
    for comp in range(2):
        full = rhs_ref[comp]
        for half in range(2):
            resid[half, comp] = dup(full, half)
            solu[half, comp] = jnp.zeros((DOF, LANES), f32)

    for mat in (CLOVER, ZDIR, YDIR, XDIR, TDIR):
        load(mat).wait()
        pack(mat)

    def copies(turn, t_to):
        t_copy = pltpu.make_async_remote_copy(
            src_ref=tsend.at[turn],
            dst_ref=trecv.at[turn],
            send_sem=send_sem.at[turn, 0],
            recv_sem=recv_sem.at[turn, 0],
            device_id=(t_to, zpos),
            device_id_type=MESH,
        )
        up_copy = pltpu.make_async_remote_copy(
            src_ref=zup_send.at[turn],
            dst_ref=zup_recv.at[turn],
            send_sem=send_sem.at[turn, 1],
            recv_sem=recv_sem.at[turn, 1],
            device_id=(tpos, z_up),
            device_id_type=MESH,
        )
        dn_copy = pltpu.make_async_remote_copy(
            src_ref=zdn_send.at[turn],
            dst_ref=zdn_recv.at[turn],
            send_sem=send_sem.at[turn, 2],
            recv_sem=recv_sem.at[turn, 2],
            device_id=(tpos, z_dn),
            device_id_type=MESH,
        )
        return t_copy, up_copy, dn_copy

    def half_sweep(turn, carry):
        half = lax.rem(turn + zpos, 2)
        other = 1 - half
        t_to = jnp.where(half == 0, t_dn, t_up)
        t_copy, up_copy, dn_copy = copies(turn, t_to)
        for comp in range(2):
            search[comp] = resid[half, comp]
            corr[comp] = jnp.zeros((DOF, LANES), f32)
            face[comp] = jnp.zeros((DOF, LANES), f32)

        def step(k, c):
            mr_step(half, k)
            return c

        lax.fori_loop(0, MR_MAX, step, 0, unroll=True)

        @pl.when(turn == 0)
        def _():
            pl.semaphore_wait(barrier, 4)

        er, ei = corr[0], corr[1]

        @pl.when(half == 0)
        def _():
            tsend[turn] = jnp.where(low, er, ei)
            t_copy.start()

        zdn_send[turn] = face_pack(jnp.where(low, er, ei))
        fr, fi = face[0], face[1]
        fr = fr + roll(fr, HALF)
        fi = fi + roll(fi, HALF)
        zup_send[turn] = face_pack(jnp.where(low, fr, fi))
        dn_copy.start()
        up_copy.start()
        store_bcast(er, ei)
        pr, pi = backward_only(half, TDIR)
        pr = pr + roll(pr, HALF)
        pi = pi + roll(pi, HALF)

        @pl.when(half == 1)
        def _():
            tsend[turn] = jnp.where(low, pr, pi)
            t_copy.start()

        for comp in range(2):
            resid[half, comp] = search[comp]
            solu[half, comp] = solu[half, comp] + corr[comp]
        face[0] = pr
        face[1] = pi

        dn_copy.wait_recv()
        zr, zi = face_unpack(zdn_recv[turn], 3)
        forward_only(other, ZDIR, zr, zi, True)

        @pl.when(half == 1)
        def _():
            forward_only(other, TDIR, corr[0], corr[1], False)

        up_copy.wait_recv()
        ur, ui = face_unpack(zup_recv[turn], 0)
        ur = ur + resid[other, 0]
        ui = ui + resid[other, 1]

        @pl.when(half == 1)
        def _():
            resid[other, 0] = ur + gather_forward(fwd_re)
            resid[other, 1] = ui + gather_forward(fwd_im)

        @pl.when(half == 0)
        def _():
            resid[other, 0] = ur + face[0]
            resid[other, 1] = ui + face[1]

        t_copy.wait_recv()
        tr, ti = split_dup(trecv[turn])

        @pl.when(half == 0)
        def _():
            forward_only(other, TDIR, tr, ti, False)
            resid[other, 0] = resid[other, 0] + gather_forward(fwd_re)
            resid[other, 1] = resid[other, 1] + gather_forward(fwd_im)

        @pl.when(half == 1)
        def _():
            resid[other, 0] = resid[other, 0] + tr
            resid[other, 1] = resid[other, 1] + ti

        return carry

    lax.fori_loop(0, HALF_SWEEPS, half_sweep, 0)

    for comp in range(2):
        sol_ref[comp] = jnp.where(low, solu[0, comp], solu[1, comp])
        res_ref[comp] = jnp.where(low, resid[0, comp], resid[1, comp])

    def drain(turn, carry):
        for copy in copies(turn, t_up):
            copy.wait_send()
        return carry

    lax.fori_loop(0, HALF_SWEEPS, drain, 0)


def write_out(sol_in, res_in, sol_hbm, res_hbm, sems):
    first = pltpu.make_async_copy(sol_in, sol_hbm, sems.at[0])
    second = pltpu.make_async_copy(res_in, res_hbm, sems.at[1])
    first.start()
    second.start()
    first.wait()
    second.wait()


def solution(mesh):
    time_count, space_count = mesh.shape["ta"], mesh.shape["sa"]
    f32 = jnp.float32
    vmem = pltpu.VMEM
    field = (2, DOF, LANES)

    def shards(rhs, links, clover, mr_steps):
        out = jax.ShapeDtypeStruct(field, f32)
        message = vmem((HALF_SWEEPS, DOF, LANES), f32)
        small = vmem((HALF_SWEEPS, 16, LANES), f32)
        sol, res = pl.pallas_call(
            functools.partial(kernel, time_count, space_count),
            out_shape=(out, out),
            in_specs=[
                pl.BlockSpec(memory_space=pltpu.HBM),
                pl.BlockSpec(memory_space=pltpu.HBM),
                pl.BlockSpec(memory_space=pltpu.HBM),
                pl.BlockSpec(memory_space=pltpu.HBM),
            ],
            out_specs=(pl.BlockSpec(memory_space=pltpu.VMEM),) * 2,
            scratch_shapes=[
                vmem((2, 5, PAIRS, 3, DOF, LANES), f32),
                vmem((5, 2, DOF, DOF, LANES), jnp.bfloat16),
                vmem((2,) + field, f32),
                vmem((2,) + field, f32),
                vmem((8, DOF, LANES), f32),
                vmem((3, 32, LANES), f32),
                vmem((PAIRS, 8, LANES), f32),
                vmem((PAIRS, 8, LANES), f32),
                message,
                small,
                small,
                message,
                small,
                small,
                pltpu.SMEM((2,), jnp.int32),
                pltpu.SemaphoreType.DMA((7,)),
                pltpu.SemaphoreType.DMA((HALF_SWEEPS, 3)),
                pltpu.SemaphoreType.DMA((HALF_SWEEPS, 3)),
            ],
            compiler_params=pltpu.CompilerParams(
                collective_id=0, has_side_effects=True, vmem_limit_bytes=40 * 2**20
            ),
        )(
            pltpu.with_memory_space_constraint(rhs.reshape(field), pltpu.HBM),
            pltpu.with_memory_space_constraint(links.reshape(4, 2, DOF, DOF, LANES), pltpu.HBM),
            pltpu.with_memory_space_constraint(clover.reshape(2, DOF, DOF, LANES), pltpu.HBM),
            pltpu.with_memory_space_constraint(mr_steps.reshape(2), pltpu.HBM),
        )
        sol, res = pl.pallas_call(
            write_out,
            out_shape=(out, out),
            in_specs=[pl.BlockSpec(memory_space=pltpu.VMEM)] * 2,
            out_specs=(pl.BlockSpec(memory_space=pltpu.HBM),) * 2,
            scratch_shapes=[pltpu.SemaphoreType.DMA((2,))],
            compiler_params=pltpu.CompilerParams(vmem_limit_bytes=40 * 2**20),
        )(sol, res)
        shape = rhs.shape
        return sol.reshape(shape), res.reshape(shape)

    placed = (
        P(None, None, None, "ta", "sa", None),
        P(None, None, None, None, "ta", "sa", None),
        P(None, None, None, "ta", "sa", None),
        P("ta", "sa", None),
    )
    return jax.shard_map(
        shards,
        mesh=mesh,
        in_specs=placed,
        out_specs=(P(None, None, None, "ta", "sa", None),) * 2,
        check_vma=False,
    )
```
